32 devices in a mesh: shard: 2 (over y), context: 4 (over x, core), tensor: 4 (over z).
Axes of the slice: x: 2, y: 2, z: 4, core: 2. Of those that a mesh axis runs over, the one named last changes fastest.
Arguments:
- inputs: bfloat16 [8, 1024, 2048], P('shard', 'context', 'tensor')
- cotangent: bfloat16 [8, 1024, 2048], P('shard', 'context', 'tensor'), may hold values from -8 to 8
- doc_lengths: int32 [8, 8], P('shard'), may hold values from 1 to 512, 1024 in all within a row
- attn_weights: float32 [4, 2048, 2048], P(None, ('shard', 'context'), 'tensor')
- mlp_weights: float32 [2, 2048, 8192], P(None, ('shard', 'context'), 'tensor'), may hold values from -0.09375 to 0.09375
- vectors: float32 [7, 2048], P(None, 'tensor')
- hidden_bias: float32 [8192], P('tensor'), may hold values from -1.5 to 1.5
- attn_moment: float32 [4, 2048, 2048], P(None, ('shard', 'context'), 'tensor'), may hold values from -5 to 5
- mlp_moment: float32 [2, 2048, 8192], P(None, ('shard', 'context'), 'tensor'), may hold values from -10 to 10
- vector_moment: float32 [7, 2048], P(None, 'tensor'), may hold values from -56 to 56
- hidden_moment: float32 [8192], P('tensor'), may hold values from -16 to 16
- attn_second: float32 [4, 2048, 2048], P(None, ('shard', 'context'), 'tensor'), may hold values from 0.8192 to 8.192
- mlp_second: float32 [2, 2048, 8192], P(None, ('shard', 'context'), 'tensor'), may hold values from 3.2768 to 32.768
- vector_second: float32 [7, 2048], P(None, 'tensor'), may hold values from 81.92 to 819.2
- hidden_second: float32 [8192], P('tensor'), may hold values from 7.3728 to 73.728
Outputs:
- output: bfloat16 [8, 1024, 2048], P('shard', 'context', 'tensor')
- input_grad: bfloat16 [8, 1024, 2048], P('shard', 'context', 'tensor')
- attn_grad: float32 [4, 2048, 2048], P(None, ('shard', 'context'), 'tensor')
- mlp_grad: float32 [2, 2048, 8192], P(None, ('shard', 'context'), 'tensor')
- vector_grad: float32 [7, 2048], P(None, 'tensor')
- hidden_grad: float32 [8192], P('tensor')
- attn_new: float32 [4, 2048, 2048], P(None, ('shard', 'context'), 'tensor')
- mlp_new: float32 [2, 2048, 8192], P(None, ('shard', 'context'), 'tensor')
- vector_new: float32 [7, 2048], P(None, 'tensor')
- hidden_new: float32 [8192], P('tensor')
- attn_moment_new: float32 [4, 2048, 2048], P(None, ('shard', 'context'), 'tensor')
- mlp_moment_new: float32 [2, 2048, 8192], P(None, ('shard', 'context'), 'tensor')
- vector_moment_new: float32 [7, 2048], P(None, 'tensor')
- hidden_moment_new: float32 [8192], P('tensor')
- attn_second_new: float32 [4, 2048, 2048], P(None, ('shard', 'context'), 'tensor')
- mlp_second_new: float32 [2, 2048, 8192], P(None, ('shard', 'context'), 'tensor')
- vector_second_new: float32 [7, 2048], P(None, 'tensor')
- hidden_second_new: float32 [8192], P('tensor')
The draws below stay inside these ranges and needn't reach their ends.
Inputs may be any that keep to these rules, and one draw needn't show every extreme that they name: `doc_lengths`: each row lists its 8 documents in order; they fill the row, and the longest in each row has 512 tokens.
All inputs are finite; a program needn't handle non-finite values.
Results may differ from the reference program's by a relative error of at most 0.006.
The reference program's roundings to bfloat16 on the way count: a program that leaves them out, or rounds other values in their place, can miss the bound.
Values may be sent and summed in bfloat16 or wider, within the bound.
A program may use at most 256 MiB of HBM per device.

```python
import math
import jax
import jax.numpy as jnp
import numpy as np
from jax import lax

D = 2048
HEADS = 32
HD = 64
ROT = 32
FF = 8192
DOCS = 8
STEP = 7
LEN = 1024
ROWS = 8
TOKENS = 8192


def draw_inputs(key, part):
    base = jax.random.normal(jax.random.fold_in(key, 1), (ROWS, LEN, D), jnp.float32)
    column = jnp.exp(jax.random.uniform(jax.random.fold_in(key, 2), (D,), jnp.float32, -1.15, 1.15))
    field = base * column
    return jnp.clip(field, -8.0, 8.0).astype(jnp.bfloat16)


def draw_attn_weights(key, part):
    inner = jax.random.normal(jax.random.fold_in(key, 1), (4, D, D), jnp.float32) * D ** (-0.5)
    outer = inner[3] * (LEN ** 0.5 / 4.0)
    stacked = jnp.stack([inner[0], inner[1], inner[2], outer])
    return stacked


def draw_vectors(key, part):
    gain = 1.0 + 0.3 * jax.random.uniform(jax.random.fold_in(key, 1), (1, D), jnp.float32, -1.0, 1.0)
    others = 0.3 * jnp.clip(jax.random.normal(jax.random.fold_in(key, 2), (6, D), jnp.float32), -4.0, 4.0)
    return jnp.concatenate([gain, others], axis=0)


def spiked(entries, own_key, source, target, blocks, factor):
    def block_of(axis_at):
        return (jnp.arange(entries.shape[axis_at]) // (entries.shape[axis_at] // blocks)).reshape((-1,) + (1,) * (entries.ndim - 1 - axis_at))

    near = jax.random.permutation(own_key, blocks)[block_of(target)]
    far = (block_of(target) + blocks // 2) % blocks
    return jnp.where((block_of(source) == near) | (block_of(source) == far), factor * entries, entries)


def block_levels(rng, dims, split, low, top_value):
    factor_of = 1.0
    for dim, blocks in split:
        steps = jax.random.uniform(jax.random.fold_in(jax.random.fold_in(rng, 6), dim), (blocks,), jnp.float32, low / len(split), top_value / len(split))
        factor_of = factor_of * jnp.repeat(jnp.exp(steps), dims[dim] // blocks).reshape((-1,) + (1,) * (len(dims) - 1 - dim))
    return factor_of


def profile(count, total, limit, skew):
    weights = [(1 << 20) // math.isqrt(standing ** skew) + 1 for standing in range(2, count + 1)]
    spare, given = total - limit - (count - 1), [1] * (count - 1)
    while spare > 0:
        movable = [i for i in range(count - 1) if given[i] < limit]
        pool, left = sum([weights[i] for i in movable]), spare
        for i in movable:
            addition = min(limit - given[i], max(1, left * weights[i] // pool), spare)
            given[i] = given[i] + addition
            spare = spare - addition
    return np.array([limit] + given)


def ragged_sizes(rng, count, total, most, skew):
    if count == 2:
        one = jax.random.randint(rng, (), max(1, total - most), min(most, total - 1) + 1)
        return jnp.stack([one, total - one])
    tallies = jnp.asarray(profile(count, total, most, skew), jnp.int32)
    pairs = (count - 1) // 2
    donor, sink = tallies[1:1 + 2 * pairs:2], tallies[2:2 + 2 * pairs:2]
    room = jnp.minimum(donor - 1, most - sink)
    shifted = jax.random.randint(jax.random.fold_in(rng, 1), (pairs,), 0, 1 << 20) % (room + 1)
    tallies = tallies.at[1:1 + 2 * pairs:2].set(donor - shifted).at[2:2 + 2 * pairs:2].set(sink + shifted)
    return tallies[jax.random.permutation(jax.random.fold_in(rng, 2), count)]


def bell_draw(key, dims, spread, limit, split=(), kind=jnp.bfloat16):
    level = block_levels(key, dims, split, -0.22, 0.18) if split else 1.0
    array = jax.random.normal(key, dims, jnp.float32) * spread * level
    return jnp.minimum(jnp.maximum(array, -limit), limit).astype(kind)


def heavy_noise(stream_key, extent, spread, reach, split, heavy, kind=jnp.bfloat16):
    entries = spread * jax.random.normal(stream_key, extent, jnp.float32)
    if split:
        entries = entries * block_levels(stream_key, extent, split, -0.22, 0.18)
    return jnp.clip(spiked(entries, jax.random.fold_in(stream_key, 3), *heavy), -reach, reach).astype(kind)


def setup_inputs(seed: int = 0) -> dict:
    seeds = jax.random.split(jax.random.key(seed), 16)
    return {
        "inputs": draw_inputs(jax.random.fold_in(seeds[15], 71), 0),
        "cotangent": heavy_noise(seeds[1], (ROWS, LEN, D), 1.0, 8.0, ((0, 2), (1, 4), (2, 4)), (1, 2, 4, 2.0)),
        "doc_lengths": jax.vmap(lambda own: ragged_sizes(own, DOCS, LEN, LEN // 2, 2))(jax.random.split(seeds[2], ROWS)).reshape((ROWS, DOCS)).astype(jnp.int32),
        "attn_weights": draw_attn_weights(jax.random.fold_in(seeds[15], 71), 0),
        "mlp_weights": bell_draw(seeds[4], (2, D, FF), (2 * D) ** -0.5, 0.09375, ((1, 8), (2, 4)), jnp.float32),
        "vectors": draw_vectors(jax.random.fold_in(seeds[15], 71), 0),
        "hidden_bias": bell_draw(seeds[6], (FF,), 0.3, 1.5, ((0, 4),), jnp.float32),
        "attn_moment": bell_draw(seeds[7], (4, D, D), (0.01 * TOKENS ** 0.5), 5.0, ((1, 8), (2, 4)), jnp.float32),
        "mlp_moment": bell_draw(seeds[8], (2, D, FF), (0.02 * TOKENS ** 0.5), 10.0, ((1, 8), (2, 4)), jnp.float32),
        "vector_moment": bell_draw(seeds[9], (7, D), (0.1 * TOKENS ** 0.5), 56.0, ((1, 4),), jnp.float32),
        "hidden_moment": bell_draw(seeds[10], (FF,), (0.03 * TOKENS ** 0.5), 16.0, ((0, 4),), jnp.float32),
        "attn_second": jnp.clip(jnp.exp(math.log(8.192) - 2.3025852 * jax.random.uniform(seeds[11], (4, D, D), jnp.float32) ** block_levels(seeds[11], (4, D, D), ((1, 8), (2, 4)), -0.2, 0.2)), 0.8192, 8.192),
        "mlp_second": jnp.clip(jnp.exp(math.log(32.768) - 2.3025852 * jax.random.uniform(seeds[12], (2, D, FF), jnp.float32) ** block_levels(seeds[12], (2, D, FF), ((1, 8), (2, 4)), -0.2, 0.2)), 3.2768, 32.768),
        "vector_second": jnp.clip(jnp.exp(math.log(819.2) - 2.3025851 * jax.random.uniform(seeds[13], (7, D), jnp.float32) ** block_levels(seeds[13], (7, D), ((1, 4),), -0.2, 0.2)), 81.92, 819.2),
        "hidden_second": jnp.clip(jnp.exp(math.log(73.728) - 2.3025851 * jax.random.uniform(seeds[14], (FF,), jnp.float32) ** block_levels(seeds[14], (FF,), ((0, 4),), -0.2, 0.2)), 7.3728, 73.728),
    }


norm_epsilon = 1e-05
first_beta = 0.9
second_beta = 0.95
adam_epsilon = 1e-08
learn_rate = 0.1
weight_decay = 0.1
rotary_base = 10000.0

@jax.custom_vjp
def low(v):
    return lax.optimization_barrier(v.astype(jnp.bfloat16)).astype(jnp.float32)

@jax.custom_vjp
def low_back(v):
    return v

def low_keep(v):
    return (low(v), None)

def low_pass(kept, grad):
    return (grad,)

def back_keep(v):
    return (v, None)

def back_low(kept, grad):
    return (low(grad),)
low.defvjp(low_keep, low_pass)
low_back.defvjp(back_keep, back_low)

def rotate(field, cosine, sine, half_rot):
    first = field[..., :half_rot]
    second = field[..., half_rot:2 * half_rot]
    return jnp.concatenate([first * cosine - second * sine, second * cosine + first * sine, field[..., 2 * half_rot:]], axis=-1)

def forward_row(x_row, attn_weights, mlp_weights, vectors, hidden_bias, doc_row, cosine, sine):
    highest = lax.Precision.HIGHEST
    length = x_row.shape[0]
    mean_val = lax.optimization_barrier(jnp.mean(x_row, axis=1, keepdims=True))
    centered = x_row - mean_val
    variance = lax.optimization_barrier(jnp.mean(centered * centered, axis=1, keepdims=True))
    normal = centered * lax.rsqrt(variance + norm_epsilon)
    normed = low(normal * low(vectors[0]) + low(vectors[1]))
    attn_low = low(attn_weights)
    mlp_low = low(mlp_weights)
    query_pre = low_back(jnp.dot(normed, attn_low[0], precision=highest) + vectors[2])
    key_pre = low_back(jnp.dot(normed, attn_low[1], precision=highest) + vectors[3])
    value_pre = jnp.dot(normed, attn_low[2], precision=highest) + vectors[4]
    grid = (length, HEADS, HD)
    queries = low(low_back(rotate(query_pre.reshape(grid), cosine, sine, ROT // 2)))
    key_rows = low(low_back(rotate(key_pre.reshape(grid), cosine, sine, ROT // 2)))
    values = low(low_back(value_pre.reshape(grid)))
    position = jnp.arange(length, dtype=jnp.int32)
    allowed = (doc_row[:, None] == doc_row[None, :]) & (position[None, :] <= position[:, None])
    scale = HD ** (-0.5)

    def one_head(parts):
        query, key_part, value_part = parts
        raw = jnp.dot(query, key_part.T, precision=highest) * scale
        scores = jnp.where(allowed, low_back(raw), -jnp.inf)
        total = jax.nn.logsumexp(scores, axis=1, keepdims=True)
        probs = low(jnp.exp(scores - total))
        return jnp.dot(probs, value_part, precision=highest)
    heads = lax.map(jax.checkpoint(one_head), (jnp.transpose(queries, (1, 0, 2)), jnp.transpose(key_rows, (1, 0, 2)), jnp.transpose(values, (1, 0, 2))))
    attended = low(low_back(heads))
    flat = jnp.transpose(attended, (1, 0, 2)).reshape(length, HEADS * HD)
    attn_out = jnp.dot(flat, attn_low[3].T, precision=highest)
    pre_act = low_back(jnp.dot(normed, mlp_low[0], precision=highest) + hidden_bias)
    hidden = low(jax.nn.gelu(pre_act, approximate=True))
    mlp_out = jnp.dot(hidden, mlp_low[1].T, precision=highest)
    return x_row + (attn_out + mlp_out) + vectors[5] + vectors[6]

def adam_update(weight, moment, second, grad):
    count = float(STEP)
    new_moment = first_beta * moment + (1.0 - first_beta) * grad
    new_second = second_beta * second + (1.0 - second_beta) * grad * grad
    moment_hat = new_moment / (1.0 - first_beta ** count)
    second_hat = new_second / (1.0 - second_beta ** count)
    new_weight = weight - learn_rate * (moment_hat / (jnp.sqrt(second_hat) + adam_epsilon) + weight_decay * weight)
    return (new_weight, new_moment, new_second)

def reference(inputs, cotangent, doc_lengths, attn_weights, mlp_weights, vectors, hidden_bias, attn_moment, mlp_moment, vector_moment, hidden_moment, attn_second, mlp_second, vector_second, hidden_second):
    ends = jnp.cumsum(doc_lengths, axis=1)
    starts = ends - doc_lengths
    index = jnp.arange(LEN, dtype=jnp.int32)
    doc_ids = lax.optimization_barrier(jnp.sum((index[None, :, None] >= ends[:, None, :]).astype(jnp.int32), axis=2))
    inside = (index[None, :, None] >= starts[:, None, :]) & (index[None, :, None] < ends[:, None, :])
    doc_start = lax.optimization_barrier(jnp.sum(jnp.where(inside, starts[:, None, :], 0), axis=2))
    position = (index[None, :] - doc_start).astype(jnp.float32)
    half_rot = ROT // 2
    freq = rotary_base ** (-(2.0 * jnp.arange(half_rot, dtype=jnp.float32)) / ROT)
    angle = position[:, :, None] * freq[None, None, :]
    cosine = jnp.cos(angle)[:, :, None, :]
    sine = jnp.sin(angle)[:, :, None, :]

    def one_row(totals, row):
        x_row, cot_row, doc_row, cos_row, sin_row = row

        def local_forward(x_full, attn_part, mlp_part, vector_part, bias_part):
            return forward_row(x_full, attn_part, mlp_part, vector_part, bias_part, doc_row, cos_row, sin_row)
        out_row, pullback = jax.vjp(local_forward, x_row.astype(jnp.float32), attn_weights, mlp_weights, vectors, hidden_bias)
        grads = pullback(cot_row.astype(jnp.float32))
        summed = tuple((total + grad for total, grad in zip(totals, grads[1:])))
        return (summed, (out_row.astype(jnp.bfloat16), grads[0].astype(jnp.bfloat16)))
    start = (jnp.zeros_like(attn_weights), jnp.zeros_like(mlp_weights), jnp.zeros_like(vectors), jnp.zeros_like(hidden_bias))
    totals, outs = lax.scan(one_row, start, (inputs, cotangent, doc_ids, cosine, sine))
    output, input_grad = outs
    attn_grad, mlp_grad, vector_grad, hidden_grad = totals
    attn_new, attn_moment_new, attn_second_new = adam_update(attn_weights, attn_moment, attn_second, attn_grad)
    mlp_new, mlp_moment_new, mlp_second_new = adam_update(mlp_weights, mlp_moment, mlp_second, mlp_grad)
    vector_new, vector_moment_new, vector_second_new = adam_update(vectors, vector_moment, vector_second, vector_grad)
    hidden_new, hidden_moment_new, hidden_second_new = adam_update(hidden_bias, hidden_moment, hidden_second, hidden_grad)
    return (output, input_grad, attn_grad, mlp_grad, vector_grad, hidden_grad, attn_new, mlp_new, vector_new, hidden_new, attn_moment_new, mlp_moment_new, vector_moment_new, hidden_moment_new, attn_second_new, mlp_second_new, vector_second_new, hidden_second_new)
```

```python
import functools

import jax
import jax.numpy as jnp
from jax import lax
from jax.experimental import pallas as pl
from jax.experimental.pallas import tpu as pltpu
from jax.sharding import PartitionSpec as P

D = 2048
HEADS = 32
HD = 64
ROT = 32
STEP = 7


norm_epsilon = 1e-05
first_beta = 0.9
second_beta = 0.95
adam_epsilon = 1e-08
learn_rate = 0.1
weight_decay = 0.1
rotary_base = 10000.0
masked_score = -1e30


def rotate(field, cosine, sine, half_rot):
    first = field[:, :, :half_rot]
    second = field[:, :, half_rot : 2 * half_rot]
    return jnp.concatenate(
        [
            first * cosine - second * sine,
            second * cosine + first * sine,
            field[:, :, 2 * half_rot :],
        ],
        axis=2,
    )


def block_scores(query_blk, key_blk, scale):
    return jnp.einsum("eq,ek->qk", query_blk, key_blk, preferred_element_type=jnp.float32) * scale


def block_mask(doc_row, q_start, k_start, block):
    q_docs = lax.dynamic_slice_in_dim(doc_row, q_start, block)
    k_docs = lax.dynamic_slice_in_dim(doc_row, k_start, block)
    offsets = jnp.arange(block, dtype=jnp.int32)
    causal = (k_start + offsets)[None, :] <= (q_start + offsets)[:, None]
    return (q_docs[:, None] == k_docs[None, :]) & causal


def block_empty(doc_row, q_start, k_start, block):
    return doc_row[k_start + block - 1] < doc_row[q_start]


def attend_item(query, key_rows, values, doc_row, block, scale):
    head_dim, length = query.shape

    def query_step(q_block, carry):
        out_acc, lse_acc = carry
        q_start = q_block * block
        query_blk = lax.dynamic_slice_in_dim(query, q_start, block, 1)

        def stats_step(k_block, state):
            k_start = k_block * block

            def stats_live(state_in):
                run_max, run_sum = state_in
                key_blk = lax.dynamic_slice_in_dim(key_rows, k_start, block, 1)
                allowed = block_mask(doc_row, q_start, k_start, block)
                scores = jnp.where(allowed, block_scores(query_blk, key_blk, scale), masked_score)
                new_max = jnp.maximum(run_max, jnp.max(scores, axis=1))
                weights = jnp.where(allowed, jnp.exp(scores - new_max[:, None]), 0.0)
                return (new_max, run_sum * jnp.exp(run_max - new_max) + jnp.sum(weights, axis=1))

            return lax.cond(
                block_empty(doc_row, q_start, k_start, block),
                lambda state_in: state_in,
                stats_live,
                state,
            )

        first_state = (
            jnp.full((block,), masked_score, jnp.float32),
            jnp.zeros((block,), jnp.float32),
        )
        run_max, run_sum = lax.fori_loop(0, q_block + 1, stats_step, first_state)
        lse_blk = run_max + jnp.log(run_sum)

        def value_step(k_block, acc):
            k_start = k_block * block

            def value_live(acc_in):
                key_blk = lax.dynamic_slice_in_dim(key_rows, k_start, block, 1)
                value_blk = lax.dynamic_slice_in_dim(values, k_start, block, 1)
                allowed = block_mask(doc_row, q_start, k_start, block)
                scores = block_scores(query_blk, key_blk, scale)
                probs = jnp.where(allowed, jnp.exp(scores - lse_blk[:, None]), 0.0).astype(
                    jnp.bfloat16
                )
                return acc_in + jnp.einsum(
                    "qk,ek->eq", probs, value_blk, preferred_element_type=jnp.float32
                )

            return lax.cond(
                block_empty(doc_row, q_start, k_start, block),
                lambda acc_in: acc_in,
                value_live,
                acc,
            )

        acc = lax.fori_loop(0, q_block + 1, value_step, jnp.zeros((head_dim, block), jnp.float32))
        out_acc = lax.dynamic_update_slice_in_dim(out_acc, acc.astype(jnp.bfloat16), q_start, 1)
        lse_acc = lax.dynamic_update_slice_in_dim(lse_acc, lse_blk, q_start, 0)
        return (out_acc, lse_acc)

    first_carry = (jnp.zeros((head_dim, length), jnp.bfloat16), jnp.zeros((length,), jnp.float32))
    return lax.fori_loop(0, length // block, query_step, first_carry)


def attend_back(query, key_rows, values, grad_out, lse, doc_row, block, scale):
    head_dim, length = query.shape

    def query_step(q_block, carry):
        grad_query, grad_key, grad_value = carry
        q_start = q_block * block
        query_blk = lax.dynamic_slice_in_dim(query, q_start, block, 1)
        gout_blk = lax.dynamic_slice_in_dim(grad_out, q_start, block, 1)
        lse_blk = lax.dynamic_slice_in_dim(lse, q_start, block, 0)

        def pieces(k_start):
            key_blk = lax.dynamic_slice_in_dim(key_rows, k_start, block, 1)
            value_blk = lax.dynamic_slice_in_dim(values, k_start, block, 1)
            allowed = block_mask(doc_row, q_start, k_start, block)
            scores = block_scores(query_blk, key_blk, scale)
            probs = jnp.where(allowed, jnp.exp(scores - lse_blk[:, None]), 0.0)
            dprobs = jnp.einsum(
                "eq,ek->qk", gout_blk, value_blk, preferred_element_type=jnp.float32
            )
            return (key_blk, probs, dprobs)

        def delta_step(k_block, delta):
            k_start = k_block * block

            def delta_live(delta_in):
                key_blk, probs, dprobs = pieces(k_start)
                return delta_in + jnp.sum(probs * dprobs, axis=1)

            return lax.cond(
                block_empty(doc_row, q_start, k_start, block),
                lambda delta_in: delta_in,
                delta_live,
                delta,
            )

        delta = lax.fori_loop(0, q_block + 1, delta_step, jnp.zeros((block,), jnp.float32))

        def grad_step(k_block, state):
            k_start = k_block * block

            def grad_live(state_in):
                query_part, key_all, value_all = state_in
                key_blk, probs, dprobs = pieces(k_start)
                dscores = (probs * (dprobs - delta[:, None])).astype(jnp.bfloat16)
                query_part = query_part + jnp.einsum(
                    "qk,ek->eq", dscores, key_blk, preferred_element_type=jnp.float32
                )
                key_add = (
                    jnp.einsum("qk,eq->ek", dscores, query_blk, preferred_element_type=jnp.float32)
                    * scale
                )
                value_add = jnp.einsum(
                    "qk,eq->ek",
                    probs.astype(jnp.bfloat16),
                    gout_blk,
                    preferred_element_type=jnp.float32,
                )
                key_all = lax.dynamic_update_slice_in_dim(
                    key_all,
                    lax.dynamic_slice_in_dim(key_all, k_start, block, 1) + key_add,
                    k_start,
                    1,
                )
                value_all = lax.dynamic_update_slice_in_dim(
                    value_all,
                    lax.dynamic_slice_in_dim(value_all, k_start, block, 1) + value_add,
                    k_start,
                    1,
                )
                return (query_part, key_all, value_all)

            return lax.cond(
                block_empty(doc_row, q_start, k_start, block),
                lambda state_in: state_in,
                grad_live,
                state,
            )

        first_state = (jnp.zeros((head_dim, block), jnp.float32), grad_key, grad_value)
        query_part, grad_key, grad_value = lax.fori_loop(0, q_block + 1, grad_step, first_state)
        grad_query = lax.dynamic_update_slice_in_dim(grad_query, query_part * scale, q_start, 1)
        return (grad_query, grad_key, grad_value)

    zero_grid = jnp.zeros((head_dim, length), jnp.float32)
    grad_query, grad_key, grad_value = lax.fori_loop(
        0, length // block, query_step, (zero_grid, zero_grid, zero_grid)
    )
    return (
        grad_query.astype(jnp.bfloat16),
        grad_key.astype(jnp.bfloat16),
        grad_value.astype(jnp.bfloat16),
    )


def adam_update(weight, moment, second, grad):
    count = float(STEP)
    new_moment = first_beta * moment + (1.0 - first_beta) * grad
    new_second = second_beta * second + (1.0 - second_beta) * grad * grad
    moment_hat = new_moment / (1.0 - first_beta**count)
    second_hat = new_second / (1.0 - second_beta**count)
    new_weight = weight - learn_rate * (
        moment_hat / (jnp.sqrt(second_hat) + adam_epsilon) + weight_decay * weight
    )
    return (new_weight, new_moment, new_second)


def body(
    inputs,
    cotangent,
    doc_lengths,
    attn_weights,
    mlp_weights,
    vectors,
    hidden_bias,
    attn_moment,
    mlp_moment,
    vector_moment,
    hidden_moment,
    attn_second,
    mlp_second,
    vector_second,
    hidden_second,
):
    sequences, local_len, width_part = inputs.shape
    n_context = lax.axis_size("context")
    n_tensor = lax.axis_size("tensor")
    heads_here = HEADS // n_tensor
    tokens_here = sequences * local_len
    length = local_len * n_context
    block = min(512, length)
    per_device = sequences * heads_here // n_context
    scale = HD ** (-0.5)
    half_rot = ROT // 2
    ends = jnp.cumsum(doc_lengths, axis=1)
    starts = ends - doc_lengths
    all_index = jnp.arange(length, dtype=jnp.int32)
    doc_ids = jnp.sum((all_index[None, :, None] >= ends[:, None, :]).astype(jnp.int32), axis=2)
    local_index = lax.axis_index("context") * local_len + jnp.arange(local_len, dtype=jnp.int32)
    inside = (local_index[None, :, None] >= starts[:, None, :]) & (
        local_index[None, :, None] < ends[:, None, :]
    )
    doc_start = jnp.sum(jnp.where(inside, starts[:, None, :], 0), axis=2)
    position = (local_index[None, :] - doc_start).astype(jnp.float32)
    freq = rotary_base ** (-(2.0 * jnp.arange(half_rot, dtype=jnp.float32)) / ROT)
    angle = freq[None, :, None] * position[:, None, :]
    cosine = jnp.cos(angle)[:, None]
    sine = jnp.sin(angle)[:, None]
    norm_low = vectors[0:2].astype(jnp.bfloat16)
    tokens_full, norm_full = (
        lax.all_gather(inputs, "tensor", axis=2, tiled=True),
        lax.all_gather(norm_low, "tensor", axis=1, tiled=True),
    )
    rows_in = tokens_full.astype(jnp.float32).reshape(tokens_here, D)
    mean_val = jnp.mean(rows_in, axis=1, keepdims=True)
    centered = rows_in - mean_val
    variance = jnp.mean(centered * centered, axis=1, keepdims=True)
    inv_std = lax.rsqrt(variance + norm_epsilon)
    normal = centered * inv_std
    gain_full = norm_full[0].astype(jnp.float32)
    normed = (normal * gain_full + norm_full[1].astype(jnp.float32)).astype(jnp.bfloat16)
    attn_full, mlp_full = (
        lax.all_gather(attn_weights.astype(jnp.bfloat16), ("shard", "context"), axis=1, tiled=True),
        lax.all_gather(mlp_weights.astype(jnp.bfloat16), ("shard", "context"), axis=1, tiled=True),
    )
    token_grid = normed.reshape(sequences, local_len, D)
    qkv_weights = attn_full[0:3].reshape(3, D, heads_here, HD)
    projected = jnp.einsum(
        "std,cdhe->cshet", token_grid, qkv_weights, preferred_element_type=jnp.float32
    )
    query_pre = projected[0] + vectors[2].reshape(heads_here, HD)[None, :, :, None]
    key_pre = projected[1] + vectors[3].reshape(heads_here, HD)[None, :, :, None]
    value_pre = projected[2] + vectors[4].reshape(heads_here, HD)[None, :, :, None]
    outgoing = jnp.stack(
        [
            rotate(query_pre, cosine, sine, half_rot),
            rotate(key_pre, cosine, sine, half_rot),
            value_pre,
        ]
    ).astype(jnp.bfloat16)
    outgoing = outgoing.reshape(3, sequences * heads_here, HD, local_len)
    attn_in = lax.all_to_all(outgoing, "context", split_axis=1, concat_axis=3, tiled=True)
    item_index = lax.axis_index("context") * per_device + jnp.arange(per_device, dtype=jnp.int32)
    item_docs = jnp.take(doc_ids, item_index // heads_here, axis=0)

    def attend_one(parts):
        query, key_part, value_part, doc_row = parts
        return attend_item(query, key_part, value_part, doc_row, block, scale)

    attn_out, lse = lax.map(attend_one, (attn_in[0], attn_in[1], attn_in[2], item_docs))
    heads_out = lax.all_to_all(attn_out, "context", split_axis=2, concat_axis=0, tiled=True)
    heads_grid = heads_out.reshape(sequences, heads_here, HD, local_len)
    out_weights = attn_full[3].reshape(D, heads_here, HD)
    branch = jnp.einsum(
        "shet,ohe->sto", heads_grid, out_weights, preferred_element_type=jnp.float32
    ).reshape(tokens_here, D)
    pre_act = jnp.dot(normed, mlp_full[0], preferred_element_type=jnp.float32) + hidden_bias
    gelu_value, gelu_back = jax.vjp(lambda field: jax.nn.gelu(field, approximate=True), pre_act)
    hidden = gelu_value.astype(jnp.bfloat16)
    branch = branch + jnp.einsum(
        "tf,of->to", hidden, mlp_full[1], preferred_element_type=jnp.float32
    )
    summed = lax.psum_scatter(branch, "tensor", scatter_dimension=1, tiled=True)
    input_rows = inputs.astype(jnp.float32).reshape(tokens_here, width_part)
    output = (
        (input_rows + summed + vectors[5] + vectors[6])
        .astype(jnp.bfloat16)
        .reshape(sequences, local_len, width_part)
    )
    grad_full = lax.all_gather(cotangent, "tensor", axis=2, tiled=True)
    grad_rows = grad_full.reshape(tokens_here, D)
    attn_back, mlp_back = (
        lax.all_gather(attn_weights.astype(jnp.bfloat16), ("shard", "context"), axis=1, tiled=True),
        lax.all_gather(mlp_weights.astype(jnp.bfloat16), ("shard", "context"), axis=1, tiled=True),
    )
    out_back = attn_back[3].reshape(D, heads_here, HD)
    grad_heads = jnp.einsum(
        "sto,ohe->shet", grad_full, out_back, preferred_element_type=jnp.float32
    ).astype(jnp.bfloat16)
    grad_heads = grad_heads.reshape(sequences * heads_here, HD, local_len)
    grad_items = lax.all_to_all(grad_heads, "context", split_axis=0, concat_axis=2, tiled=True)

    def attend_grad(parts):
        query, key_part, value_part, gout, lse_row, doc_row = parts
        return attend_back(query, key_part, value_part, gout, lse_row, doc_row, block, scale)

    grad_query_item, grad_key_item, grad_value_item = lax.map(
        attend_grad, (attn_in[0], attn_in[1], attn_in[2], grad_items, lse, item_docs)
    )
    grads_back = lax.all_to_all(
        jnp.stack([grad_query_item, grad_key_item, grad_value_item]),
        "context",
        split_axis=3,
        concat_axis=1,
        tiled=True,
    )
    grad_grid = grads_back.reshape(3, sequences, heads_here, HD, local_len)
    grad_query = rotate(grad_grid[0].astype(jnp.float32), cosine, -sine, half_rot).astype(
        jnp.bfloat16
    )
    grad_key = rotate(grad_grid[1].astype(jnp.float32), cosine, -sine, half_rot).astype(
        jnp.bfloat16
    )
    grad_proj = jnp.stack([grad_query, grad_key, grad_grid[2]])
    qkv_back = attn_back[0:3].reshape(3, D, heads_here, HD)
    qkv_grad = jnp.einsum(
        "std,cshet->cdhe", token_grid, grad_proj, preferred_element_type=jnp.float32
    ).reshape(3, D, width_part)
    normed_grad = jnp.einsum(
        "cshet,cdhe->std", grad_proj, qkv_back, preferred_element_type=jnp.float32
    ).reshape(tokens_here, D)
    out_grad = jnp.einsum(
        "sto,shet->ohe", grad_full, heads_grid, preferred_element_type=jnp.float32
    ).reshape(D, width_part)
    hidden_act_grad = jnp.dot(grad_rows, mlp_back[1], preferred_element_type=jnp.float32)
    pre_grad = gelu_back(hidden_act_grad)[0].astype(jnp.bfloat16)
    second_grad = jnp.einsum("to,tf->of", grad_rows, hidden, preferred_element_type=jnp.float32)
    first_grad = jnp.einsum("td,tf->df", normed, pre_grad, preferred_element_type=jnp.float32)
    normed_grad = normed_grad + jnp.einsum(
        "tf,df->td", pre_grad, mlp_back[0], preferred_element_type=jnp.float32
    )
    norm_stats = jnp.stack([jnp.sum(normed_grad * normal, axis=0), jnp.sum(normed_grad, axis=0)])
    scaled = normed_grad * gain_full
    input_part = inv_std * (
        scaled
        - jnp.mean(scaled, axis=1, keepdims=True)
        - normal * jnp.mean(scaled * normal, axis=1, keepdims=True)
    )
    input_slice, norm_slice = (
        lax.psum_scatter(input_part, "tensor", scatter_dimension=1, tiled=True),
        lax.psum_scatter(norm_stats, "tensor", scatter_dimension=1, tiled=True),
    )
    cot_rows = cotangent.astype(jnp.float32).reshape(tokens_here, width_part)
    input_grad = (
        (cot_rows + input_slice).astype(jnp.bfloat16).reshape(sequences, local_len, width_part)
    )
    cot_total = jnp.sum(cot_rows, axis=0)
    query_bias_grad = jnp.sum(grad_query.astype(jnp.float32), axis=(0, 3)).reshape(width_part)
    key_bias_grad = jnp.sum(grad_key.astype(jnp.float32), axis=(0, 3)).reshape(width_part)
    value_bias_grad = jnp.sum(grad_grid[2].astype(jnp.float32), axis=(0, 3)).reshape(width_part)
    local_vectors = jnp.stack(
        [
            norm_slice[0],
            norm_slice[1],
            query_bias_grad,
            key_bias_grad,
            value_bias_grad,
            cot_total,
            cot_total,
        ]
    )
    local_hidden = jnp.sum(pre_grad.astype(jnp.float32), axis=0)
    vector_grad, hidden_grad = lax.psum((local_vectors, local_hidden), ("shard", "context"))
    attn_local = jnp.concatenate([qkv_grad, out_grad[None]], axis=0)
    mlp_local = jnp.stack([first_grad, second_grad])
    attn_grad, mlp_grad = (
        lax.psum_scatter(attn_local, ("shard", "context"), scatter_dimension=1, tiled=True),
        lax.psum_scatter(mlp_local, ("shard", "context"), scatter_dimension=1, tiled=True),
    )
    attn_new, attn_moment_new, attn_second_new = adam_update(
        attn_weights, attn_moment, attn_second, attn_grad
    )
    mlp_new, mlp_moment_new, mlp_second_new = adam_update(
        mlp_weights, mlp_moment, mlp_second, mlp_grad
    )
    vector_new, vector_moment_new, vector_second_new = adam_update(
        vectors, vector_moment, vector_second, vector_grad
    )
    hidden_new, hidden_moment_new, hidden_second_new = adam_update(
        hidden_bias, hidden_moment, hidden_second, hidden_grad
    )
    return (
        output,
        input_grad,
        attn_grad,
        mlp_grad,
        vector_grad,
        hidden_grad,
        attn_new,
        mlp_new,
        vector_new,
        hidden_new,
        attn_moment_new,
        mlp_moment_new,
        vector_moment_new,
        hidden_moment_new,
        attn_second_new,
        mlp_second_new,
        vector_second_new,
        hidden_second_new,
    )


def attention_kernel(
    first_ref,
    q_ref,
    k_ref,
    v_ref,
    gout_ref,
    cos_ref,
    low_ref,
    high_ref,
    start_ref,
    out_ref,
    gq_ref,
    gk_ref,
    gv_ref,
    key_cat,
    value_cat,
    raw,
    dprob,
    gk_acc,
    gv_acc,
    *,
    block,
    steps,
    scale,
    half_rot,
):
    row, step = pl.program_id(0), pl.program_id(2)
    pair = q_ref.shape[1]
    lane_low = lax.broadcasted_iota(jnp.int32, (block, pair), 1) < pair // 2
    contract_last = (((1,), (1,)), ((), ()))
    contract_first = (((0,), (0,)), ((), ()))
    plain = (((1,), (0,)), ((), ()))

    def dot(a, b, dims):
        return lax.dot_general(a, b, dims, preferred_element_type=jnp.float32)

    def turn(field, start, sign):
        rows = pl.ds(start, block)
        return (
            field * cos_ref[rows, :]
            + sign * (pltpu.roll(field, pair - half_rot, 1) * low_ref[rows, :])
            + sign * (pltpu.roll(field, half_rot, 1) * high_ref[rows, :])
        )

    @pl.when(step == 0)
    def _():
        gk_acc[...] = jnp.zeros_like(gk_acc)
        gv_acc[...] = jnp.zeros_like(gv_acc)

        @pl.loop(0, steps)
        def _(j):
            at = pl.multiple_of(j * block, block)
            keys = turn(k_ref[pl.ds(at, block), :], at, 1.0)
            values = v_ref[pl.ds(at, block), :]
            for half in range(2):
                keep = lane_low if half == 0 else jnp.logical_not(lane_low)
                rows = pl.ds(pl.multiple_of(2 * at, 2 * block) + half * block, block)
                key_cat[rows, :] = jnp.where(keep, keys, 0.0).astype(jnp.bfloat16)
                value_cat[rows, :] = jnp.where(keep, values, 0.0).astype(jnp.bfloat16)

    q_at = pl.multiple_of(step * block, block)
    queries = turn(q_ref[...], q_at, 1.0).astype(jnp.bfloat16)
    queries = (queries.astype(jnp.float32) * scale).astype(jnp.bfloat16)
    gout = gout_ref[...]
    first = first_ref[row * steps + step]
    begin = start_ref[...]
    q_pos = q_at + lax.broadcasted_iota(jnp.int32, (block, block), 0)
    k_lane = lax.broadcasted_iota(jnp.int32, (block, block), 1)

    def rows_of(j):
        return pl.ds(pl.multiple_of(j * (2 * block), 2 * block), 2 * block)

    def score_step(j, tops):
        scores = dot(queries, key_cat[rows_of(j), :], contract_last)
        k_pos = j * block + k_lane
        allowed = (k_pos <= q_pos) & (k_pos >= begin)
        new_tops = []
        for half in range(2):
            part = jnp.where(allowed, scores[:, half * block : (half + 1) * block], -3e38)
            raw[j, :, half * block : (half + 1) * block] = part
            new_tops.append(jnp.maximum(tops[half], jnp.max(part, axis=1, keepdims=True)))
        return tuple(new_tops)

    low_start = jnp.full((block, 1), -3e38, jnp.float32)
    tops = lax.fori_loop(first, step + 1, score_step, (low_start, low_start))

    def weight_step(j, sums):
        dp = dot(gout, value_cat[rows_of(j), :], contract_last)
        dprob[j] = dp
        new_sums = []
        for half in range(2):
            cols = slice(half * block, (half + 1) * block)
            weights = jnp.exp(raw[j, :, cols] - tops[half])
            raw[j, :, cols] = weights
            new_sums.append(sums[2 * half] + jnp.sum(weights, axis=1, keepdims=True))
            new_sums.append(
                sums[2 * half + 1] + jnp.sum(weights * dp[:, cols], axis=1, keepdims=True)
            )
        return tuple(new_sums)

    zero = jnp.zeros((block, 1), jnp.float32)
    sums = lax.fori_loop(first, step + 1, weight_step, (zero,) * 4)
    inverse = [1.0 / sums[0], 1.0 / sums[2]]
    delta = [sums[1] * inverse[0], sums[3] * inverse[1]]

    def grad_step(j, carry):
        out_acc, gq_acc = carry
        probs, dscores = [], []
        for half in range(2):
            cols = slice(half * block, (half + 1) * block)
            full = raw[j, :, cols] * inverse[half]
            probs.append(full.astype(jnp.bfloat16))
            dscores.append((full * (dprob[j, :, cols] - delta[half])).astype(jnp.bfloat16))
        probs = jnp.concatenate(probs, axis=1)
        dscores = jnp.concatenate(dscores, axis=1)
        rows = rows_of(j)
        out_acc = out_acc + dot(probs, value_cat[rows, :], plain)
        gq_acc = gq_acc + dot(dscores, key_cat[rows, :], plain)
        gk_acc[rows, :] += dot(dscores, queries, contract_first)
        gv_acc[rows, :] += dot(probs, gout, contract_first)
        return (out_acc, gq_acc)

    blank = jnp.zeros((block, pair), jnp.float32)
    out_acc, gq_acc = lax.fori_loop(first, step + 1, grad_step, (blank, blank))
    out_ref[...] = out_acc.astype(jnp.bfloat16)
    gq_low = (gq_acc * scale).astype(jnp.bfloat16).astype(jnp.float32)
    gq_ref[...] = turn(gq_low, q_at, -1.0).astype(jnp.bfloat16)

    @pl.when(step == steps - 1)
    def _():
        @pl.loop(0, steps)
        def _(j):
            at = pl.multiple_of(j * block, block)
            top = pl.ds(pl.multiple_of(2 * at, 2 * block), block)
            bottom = pl.ds(pl.multiple_of(2 * at, 2 * block) + block, block)
            gk = jnp.where(lane_low, gk_acc[top, :], gk_acc[bottom, :])
            gk_low = gk.astype(jnp.bfloat16).astype(jnp.float32)
            gk_ref[pl.ds(at, block), :] = turn(gk_low, at, -1.0).astype(jnp.bfloat16)
            gv_ref[pl.ds(at, block), :] = jnp.where(
                lane_low, gv_acc[top, :], gv_acc[bottom, :]
            ).astype(jnp.bfloat16)


def attention(qkv_pre, gout, tables, begin, first, rows, length, block):
    width = gout.shape[1]
    pair = 2 * HD
    pairs = width // pair
    steps = length // block
    cosine, low, high = tables
    whole = pl.BlockSpec((length, pair), lambda r, h, i, f: (r, h))
    keys = pl.BlockSpec((length, pair), lambda r, h, i, f: (r, pairs + h))
    values = pl.BlockSpec((length, pair), lambda r, h, i, f: (r, 2 * pairs + h))
    part = pl.BlockSpec((block, pair), lambda r, h, i, f: (r * steps + i, h))
    table = pl.BlockSpec((length, pair), lambda r, h, i, f: (r, 0))
    shape = jax.ShapeDtypeStruct((rows * length, width), jnp.bfloat16)
    return pl.pallas_call(
        functools.partial(
            attention_kernel, block=block, steps=steps, scale=HD ** (-0.5), half_rot=ROT // 2
        ),
        out_shape=(shape,) * 4,
        grid_spec=pltpu.PrefetchScalarGridSpec(
            num_scalar_prefetch=1,
            grid=(rows, pairs, steps),
            in_specs=[
                part,
                keys,
                values,
                part,
                table,
                table,
                table,
                pl.BlockSpec((block, 1), lambda r, h, i, f: (r * steps + i, 0)),
            ],
            out_specs=[part, part, whole, whole],
            scratch_shapes=[
                pltpu.VMEM((2 * length, pair), jnp.bfloat16),
                pltpu.VMEM((2 * length, pair), jnp.bfloat16),
                pltpu.VMEM((steps, block, 2 * block), jnp.float32),
                pltpu.VMEM((steps, block, 2 * block), jnp.float32),
                pltpu.VMEM((2 * length, pair), jnp.float32),
                pltpu.VMEM((2 * length, pair), jnp.float32),
            ],
        ),
        compiler_params=pltpu.CompilerParams(
            dimension_semantics=("arbitrary", "arbitrary", "arbitrary")
        ),
        cost_estimate=pl.CostEstimate(
            flops=rows * width * length * length * 8,
            bytes_accessed=rows * length * width * 30,
            transcendentals=rows * pairs * length * length,
        ),
    )(first, qkv_pre, qkv_pre, qkv_pre, gout, cosine, low, high, begin)


MESH = pl.DeviceIdType.MESH


def flipped(index, bits):
    bit = 1
    while bit <= bits:
        if bits & bit:
            index = index + bit - 2 * bit * ((index // bit) % 2)
        bit *= 2
    return index


def gather_kernel(
    x_ref,
    g_ref,
    norm_ref,
    x_out,
    g_out,
    normed_out,
    normed_halves,
    g_halves,
    mean_out,
    inv_out,
    gain_out,
    x_buf,
    g_buf,
    normed_buf,
    normed_parts,
    g_parts,
    norm_all,
    own_sem,
    send_a,
    recv_a,
    send_n,
    recv_n,
    send_r,
    recv_r,
    send_l,
    recv_l,
    out_sem,
    *,
    n_context,
    n_tensor,
    n_block,
    rows,
    strip,
):
    c, z = lax.axis_index("context"), lax.axis_index("tensor")
    core = c % 2
    local_len, width = x_ref.shape[1:]
    length = local_len * n_context
    sources, buffers = (x_ref, g_ref), (x_buf, g_buf)

    def peer(k):
        return flipped(c, k)

    barrier = pltpu.get_barrier_semaphore()
    for k in range(1, n_context):
        pl.semaphore_signal(barrier, inc=1, device_id={"context": peer(k)}, device_id_type=MESH)
    for k in range(1, n_tensor):
        pl.semaphore_signal(
            barrier, inc=1, device_id={"tensor": (z + k) % n_tensor}, device_id_type=MESH
        )
    pl.semaphore_wait(barrier, n_context + n_tensor - 2)

    def at(r, chunk):
        return pl.ds(pl.multiple_of(r * length + chunk * local_len, local_len), local_len)

    def piece(f, r, chunk, origin):
        return buffers[f].at[at(r, chunk), pl.ds(pl.multiple_of(origin * width, width), width)]

    def own_copy(f, r):
        return pltpu.make_async_copy(
            sources[f].at[c * rows + r], piece(f, r, c, z), own_sem.at[f, r]
        )

    own_norm = pltpu.make_async_copy(norm_ref, norm_all.at[z], own_sem.at[2, 0])

    def swap(f, r, k):
        return pltpu.make_async_remote_copy(
            src_ref=sources[f].at[peer(k) * rows + r],
            dst_ref=piece(f, r, c, z),
            send_sem=send_a.at[f, k - 1, r],
            recv_sem=recv_a.at[f, k - 1, r],
            device_id={"context": peer(k)},
            device_id_type=MESH,
        )

    def norm_copy(k):
        return pltpu.make_async_remote_copy(
            src_ref=norm_ref,
            dst_ref=norm_all.at[z],
            send_sem=send_n.at[k - 1],
            recv_sem=recv_n.at[k - 1],
            device_id={"tensor": (z + k) % n_tensor},
            device_id_type=MESH,
        )

    def hop(f, r, k, d, side, step):
        origin = z - d if side > 0 else z + d
        sends, recvs = (send_r, recv_r) if side > 0 else (send_l, recv_l)
        block = piece(f, r, peer(k), origin)
        return pltpu.make_async_remote_copy(
            src_ref=block,
            dst_ref=block,
            send_sem=sends.at[f, d - step, k, r],
            recv_sem=recvs.at[f, d - step, k, r],
            device_id={"tensor": z + side * (1 - step)},
            device_id_type=MESH,
        )

    def has(d, side):
        return z >= d if side > 0 else z + d <= n_tensor - 1

    def more(side):
        return z < n_tensor - 1 if side > 0 else z > 0

    for f in range(2):
        for r in range(rows):
            own_copy(f, r).start()
        if f == 0:
            own_norm.start()
        for k in range(1, n_context):
            for r in range(rows):
                swap(f, r, k).start()
        if f == 0:
            for k in range(1, n_tensor):
                norm_copy(k).start()
    own_norm.wait()
    for k in range(1, n_tensor):
        norm_copy(k).wait_recv()

    gain = jnp.concatenate([norm_all[j, 0:1, :] for j in range(n_tensor)], axis=1)
    shift = jnp.concatenate([norm_all[j, 1:2, :] for j in range(n_tensor)], axis=1)
    gain, shift = gain.astype(jnp.float32), shift.astype(jnp.float32)
    gain_out[...] = gain

    span = x_buf.shape[1] // n_block

    def store_parts(parts, lines, value):
        for b in range(n_block):
            cols = slice((b // 2) * span, (b // 2 + 1) * span)
            parts[(b + core) % 2, lines, cols] = value[:, b * span : (b + 1) * span]

    def finish_x(base):
        @pl.loop(0, local_len // strip)
        def _(step):
            lines = pl.ds(pl.multiple_of(base + step * strip, strip), strip)
            field = x_buf[lines, :].astype(jnp.float32)
            mean_val = jnp.mean(field, axis=1, keepdims=True)
            centered = field - mean_val
            variance = jnp.mean(centered * centered, axis=1, keepdims=True)
            inv_std = lax.rsqrt(variance + norm_epsilon)
            normed = ((centered * inv_std) * gain + shift).astype(jnp.bfloat16)
            normed_buf[lines, :] = normed
            store_parts(normed_parts, lines, normed)
            mean_out[lines, :] = mean_val
            inv_out[lines, :] = inv_std

    def finish_g(base):
        @pl.loop(0, local_len // strip)
        def _(step):
            lines = pl.ds(pl.multiple_of(base + step * strip, strip), strip)
            store_parts(g_parts, lines, g_buf[lines, :])

    def results(f, r, k):
        lines = at(r, peer(k))
        if f == 0:
            pairs = [
                (x_buf.at[lines], x_out.at[lines]),
                (normed_buf.at[lines], normed_out.at[lines]),
                (normed_parts.at[0, lines], normed_halves.at[0, lines]),
                (normed_parts.at[1, lines], normed_halves.at[1, lines]),
            ]
        else:
            pairs = [
                (g_buf.at[lines], g_out.at[lines]),
                (g_parts.at[0, lines], g_halves.at[0, lines]),
                (g_parts.at[1, lines], g_halves.at[1, lines]),
            ]
        return [
            pltpu.make_async_copy(src, dst, out_sem.at[f, k, r, i])
            for i, (src, dst) in enumerate(pairs)
        ]

    order = [(f, r, k) for f in range(2) for k in range(n_context) for r in range(rows)]
    for f, r, k in order:
        for d in range(n_tensor):
            if d == 0:
                if k == 0:
                    own_copy(f, r).wait()
                else:
                    swap(f, r, k).wait_recv()
            for side in (1, -1):
                if d > 0:

                    @pl.when(has(d, side))
                    def _():
                        hop(f, r, k, d, side, 1).wait_recv()

                if d < n_tensor - 1:

                    @pl.when(has(d, side) & more(side))
                    def _():
                        hop(f, r, k, d, side, 0).start()

        base = r * length + peer(k) * local_len
        if f == 0:
            finish_x(base)
        else:
            finish_g(base)
        for copy in results(f, r, k):
            copy.start()

    for f, r, k in order:
        for d in range(n_tensor - 1):
            for side in (1, -1):

                @pl.when(has(d, side) & more(side))
                def _():
                    hop(f, r, k, d, side, 0).wait_send()

        if k > 0:
            swap(f, r, k).wait_send()
        for copy in results(f, r, k):
            copy.wait()
    for k in range(1, n_tensor):
        norm_copy(k).wait_send()


def gather_inputs(inputs, cotangent, norm_low, n_context, n_tensor, n_block):
    sequences, local_len, width = inputs.shape
    rows = sequences // n_context
    tokens = sequences * local_len
    full = width * n_tensor
    wide, low = jnp.float32, jnp.bfloat16
    dma = pltpu.SemaphoreType.DMA
    inside = pl.BlockSpec(memory_space=pltpu.VMEM)
    outside = pl.BlockSpec(memory_space=pl.ANY)
    hops = (2, n_tensor - 1, n_context, rows)
    return pl.pallas_call(
        functools.partial(
            gather_kernel,
            n_context=n_context,
            n_tensor=n_tensor,
            n_block=n_block,
            rows=rows,
            strip=min(32, local_len),
        ),
        out_shape=(
            jax.ShapeDtypeStruct((tokens, full), low),
            jax.ShapeDtypeStruct((tokens, full), low),
            jax.ShapeDtypeStruct((tokens, full), low),
            jax.ShapeDtypeStruct((2, tokens, full // 2), low),
            jax.ShapeDtypeStruct((2, tokens, full // 2), low),
            jax.ShapeDtypeStruct((tokens, 1), wide),
            jax.ShapeDtypeStruct((tokens, 1), wide),
            jax.ShapeDtypeStruct((1, full), wide),
        ),
        in_specs=[inside] * 3,
        out_specs=(outside,) * 5 + (inside,) * 3,
        scratch_shapes=[
            pltpu.VMEM((tokens, full), low),
            pltpu.VMEM((tokens, full), low),
            pltpu.VMEM((tokens, full), low),
            pltpu.VMEM((2, tokens, full // 2), low),
            pltpu.VMEM((2, tokens, full // 2), low),
            pltpu.VMEM((n_tensor, 2, width), low),
            dma((3, rows)),
            dma((2, n_context - 1, rows)),
            dma((2, n_context - 1, rows)),
            dma((n_tensor - 1,)),
            dma((n_tensor - 1,)),
            dma(hops),
            dma(hops),
            dma(hops),
            dma(hops),
            dma((2, n_context, rows, 4)),
        ],
        compiler_params=pltpu.CompilerParams(collective_id=0, has_side_effects=True),
    )(inputs, cotangent, norm_low)


def total_kernel(
    stats_ref,
    rest_ref,
    out_ref,
    parts,
    every,
    send_z,
    recv_z,
    send_p,
    recv_p,
    *,
    n_shard,
    n_context,
    n_tensor,
):
    y, c, z = lax.axis_index("shard"), lax.axis_index("context"), lax.axis_index("tensor")
    me = y * n_context + c
    group = n_shard * n_context
    width = out_ref.shape[1]
    kept = stats_ref.shape[1]

    barrier = pltpu.get_barrier_semaphore()
    for k in range(1, n_tensor):
        pl.semaphore_signal(
            barrier, inc=1, device_id={"tensor": (z + k) % n_tensor}, device_id_type=MESH
        )

    def place(k):
        other = (me + k) % group
        return {"shard": other // n_context, "context": other % n_context}

    for k in range(1, group):
        pl.semaphore_signal(barrier, inc=1, device_id=place(k), device_id_type=MESH)
    pl.semaphore_wait(barrier, n_tensor + group - 2)

    def slice_copy(k):
        return pltpu.make_async_remote_copy(
            src_ref=stats_ref.at[(z + k) % n_tensor],
            dst_ref=parts.at[k],
            send_sem=send_z.at[k],
            recv_sem=recv_z.at[k],
            device_id={"tensor": (z + k) % n_tensor},
            device_id_type=MESH,
        )

    for k in range(1, n_tensor):
        slice_copy(k).start()
    every[me, kept:, :] = rest_ref[...]
    total = stats_ref[z]
    for k in range(1, n_tensor):
        slice_copy(k).wait_recv()
        total = total + parts[k]
    every[me, 0:kept, :] = total

    def spread(k):
        return pltpu.make_async_remote_copy(
            src_ref=every.at[me],
            dst_ref=every.at[me],
            send_sem=send_p.at[k],
            recv_sem=recv_p.at[k],
            device_id=place(k),
            device_id_type=MESH,
        )

    def spread_from(k):
        other = (me + group - k) % group
        return pltpu.make_async_remote_copy(
            src_ref=every.at[other],
            dst_ref=every.at[other],
            send_sem=send_p.at[k],
            recv_sem=recv_p.at[k],
            device_id=place(k),
            device_id_type=MESH,
        )

    for k in range(1, group):
        spread(k).start()
    for k in range(1, group):
        spread_from(k).wait_recv()
    total = every[0]
    for j in range(1, group):
        total = total + every[j]
    out_ref[...] = total
    for k in range(1, n_tensor):
        slice_copy(k).wait_send()
    for k in range(1, group):
        spread(k).wait_send()


def total_vectors(stats, rest, n_shard, n_context, n_tensor):
    kept, (more, width) = stats.shape[1], rest.shape
    group = n_shard * n_context
    dma = pltpu.SemaphoreType.DMA
    inside = pl.BlockSpec(memory_space=pltpu.VMEM)
    return pl.pallas_call(
        functools.partial(
            total_kernel, n_shard=n_shard, n_context=n_context, n_tensor=n_tensor
        ),
        out_shape=jax.ShapeDtypeStruct((kept + more, width), jnp.float32),
        in_specs=[inside] * 2,
        out_specs=inside,
        scratch_shapes=[
            pltpu.VMEM((n_tensor, kept, width), jnp.float32),
            pltpu.VMEM((group, kept + more, width), jnp.float32),
            dma((n_tensor,)),
            dma((n_tensor,)),
            dma((group,)),
            dma((group,)),
        ],
        compiler_params=pltpu.CompilerParams(collective_id=1, has_side_effects=True),
    )(stats, rest)


def permute(field, axis, pairs):
    return lax.ppermute(field, axis, pairs)


def ring_shift(field, axis, size, k):
    return lax.ppermute(field, axis, [(i, (i + k) % size) for i in range(size)])


def pick(field, index, axis):
    return lax.dynamic_index_in_dim(field, index, axis, keepdims=False)


def fast_body(
    inputs,
    cotangent,
    doc_lengths,
    attn_weights,
    mlp_weights,
    vectors,
    hidden_bias,
    attn_moment,
    mlp_moment,
    vector_moment,
    hidden_moment,
    attn_second,
    mlp_second,
    vector_second,
    hidden_second,
):
    sequences, local_len, width = inputs.shape
    n_context, n_tensor = lax.axis_size("context"), lax.axis_size("tensor")
    n_shard = lax.axis_size("shard")
    rows = sequences // n_context
    length = local_len * n_context
    tokens = rows * length
    block = min(256, length)
    half_rot = ROT // 2
    low_type = jnp.bfloat16
    wide = jnp.float32
    at_tensor, at_context = lax.axis_index("tensor"), lax.axis_index("context")
    at_y, at_x, at_core = lax.axis_index("shard"), at_context // 2, at_context % 2
    flip_core = [(i, i ^ 1) for i in range(n_context)]
    flip_x = [(i, i ^ 2) for i in range(n_context)]
    flip_y = [(i, i ^ 1) for i in range(n_shard)]

    def after(field, *others):
        return lax.optimization_barrier((field,) + others)[0]

    def dot(a, b, left, right):
        return lax.dot_general(
            a, b, (((left,), (right,)), ((), ())), preferred_element_type=wide
        )

    attn_low = jnp.concatenate([attn_weights[i] for i in range(4)], axis=1).astype(low_type)
    attn_full = lax.all_gather(attn_low, ("shard", "context"), axis=0, tiled=True)
    mlp_full = lax.all_gather(
        mlp_weights.astype(low_type), ("shard", "context"), axis=1, tiled=True
    )
    w_qkv, w_out = attn_full[:, : 3 * width], attn_full[:, 3 * width :]
    w_up, w_down = mlp_full[0], mlp_full[1]

    x_full, g_full, normed, normed_halves, g_halves, mean_val, inv_std, gain_full = gather_inputs(
        inputs,
        cotangent,
        vectors[0:2].astype(low_type),
        n_context,
        n_tensor,
        n_shard * n_context,
    )

    ends = jnp.cumsum(doc_lengths, axis=1)
    my_ends = lax.dynamic_slice_in_dim(ends, at_context * rows, rows, 0)
    index = jnp.arange(length, dtype=jnp.int32)
    doc_start = jnp.max(
        jnp.where(index[None, :, None] >= my_ends[:, None, :], my_ends[:, None, :], 0), axis=2
    )
    first = (doc_start[:, ::block] // block).reshape(-1)
    begin = doc_start.reshape(tokens, 1)
    position = (index[None, :] - doc_start).astype(wide).reshape(tokens, 1)
    lane = jnp.arange(2 * HD, dtype=jnp.int32) % HD
    freq = rotary_base ** (-(2.0 * (lane % half_rot).astype(wide)) / ROT)
    angle = position * freq[None, :]
    cosine, sine = jnp.cos(angle), jnp.sin(angle)
    tables = (
        jnp.where(lane < ROT, cosine, 1.0),
        jnp.where(lane < half_rot, -sine, 0.0),
        jnp.where((lane >= half_rot) & (lane < ROT), sine, 0.0),
    )

    qkv_pre = dot(normed, w_qkv, 1, 0) + vectors[2:5].reshape(3 * width)
    gout = dot(g_full, w_out, 1, 0).astype(low_type)
    pre_act = dot(normed, w_up, 1, 0) + hidden_bias
    gelu_value, gelu_back = jax.vjp(lambda field: jax.nn.gelu(field, approximate=True), pre_act)
    hidden = gelu_value.astype(low_type)

    attended, g_query, g_key, g_value = attention(
        qkv_pre, gout, tables, begin, first, rows, length, block
    )
    g_qkv = jnp.concatenate([g_query, g_key, g_value], axis=1)

    def scatter_features(field):
        return lax.psum_scatter(field, "tensor", scatter_dimension=1, tiled=True).astype(wide)

    def own_features(field):
        return lax.dynamic_slice_in_dim(field, at_tensor * width, width, 1).astype(wide)

    def back_rows(field):
        pieces = field.reshape(rows, n_context, local_len, width)
        result = jnp.zeros((n_context, rows, local_len, width), field.dtype)
        for k in range(n_context):
            piece = pick(pieces, at_context ^ k, 1)
            if k > 0:
                piece = permute(piece, "context", [(i, i ^ k) for i in range(n_context)])
            result = lax.dynamic_update_index_in_dim(result, piece, at_context ^ k, 0)
        return result.reshape(sequences, local_len, width)

    branch = (dot(attended, w_out, 1, 1) + dot(hidden, w_down, 1, 1)).astype(low_type)
    summed = scatter_features(branch)
    output = back_rows(
        (own_features(x_full) + summed + vectors[5] + vectors[6]).astype(low_type)
    )

    g_late = after(g_full, branch)
    pre_grad = gelu_back(dot(g_late, w_down, 1, 0))[0].astype(low_type)

    def reduce_rows(parts, right):
        mine, other = parts
        n = right.shape[1]
        half = n // 2
        sent = dot(other, right, 0, 0).astype(low_type)
        chip = (dot(mine, right, 0, 0) + permute(sent, "context", flip_core)).astype(low_type)
        chip = chip.reshape(n_shard, n_context // 2, -1, n)
        left, right_part = chip[..., :half], chip[..., half:]
        from_x = permute(pick(left, 1 - at_x, 1), "context", flip_x)
        from_y = permute(pick(right_part, 1 - at_y, 0), "shard", flip_y)
        left, right_part = pick(left, at_x, 1), pick(right_part, at_y, 0)

        def both(a, b, where):
            return pick(a, where, 0).astype(wide) + pick(b, where, 0).astype(wide)

        next_y = permute(both(left, from_x, 1 - at_y).astype(low_type), "shard", flip_y)
        next_x = permute(both(right_part, from_y, 1 - at_x).astype(low_type), "context", flip_x)
        return jnp.concatenate(
            [both(left, from_x, at_y) + next_y, both(right_part, from_y, at_x) + next_x], axis=1
        )

    down_grad = reduce_rows(after(g_halves, pre_grad), hidden)
    up_grad = reduce_rows(normed_halves, pre_grad)

    normed_grad = dot(pre_grad, w_up, 1, 1) + dot(g_qkv, w_qkv, 1, 1)
    normal = (x_full.astype(wide) - mean_val) * inv_std
    norm_stats = jnp.stack([jnp.sum(normed_grad * normal, axis=0), jnp.sum(normed_grad, axis=0)])
    scaled = normed_grad * gain_full
    input_part = (
        inv_std
        * (
            scaled
            - jnp.mean(scaled, axis=1, keepdims=True)
            - normal * jnp.mean(scaled * normal, axis=1, keepdims=True)
        )
    ).astype(low_type)
    g_qkv_late = after(g_qkv, input_part)
    qkv_grad = reduce_rows(normed_halves, g_qkv_late)
    out_grad = reduce_rows(g_halves, after(attended, g_qkv_late))

    input_slice = scatter_features(input_part)
    g_own = own_features(g_full)
    input_grad = back_rows((g_own + input_slice).astype(low_type))

    stats_grid = norm_stats.reshape(2, n_tensor, width).transpose(1, 0, 2)
    rest = jnp.concatenate(
        [
            jnp.sum(g_qkv.astype(wide), axis=0).reshape(3, width),
            jnp.sum(g_own, axis=0)[None],
            jnp.sum(pre_grad.astype(wide), axis=0).reshape(-1, width),
        ]
    )
    totals = total_vectors(stats_grid, rest, n_shard, n_context, n_tensor)
    vector_grad = jnp.concatenate([totals[0:6], totals[5:6]])
    hidden_grad = totals[6:].reshape(-1)

    attn_grad = jnp.stack(
        [qkv_grad[:, i * width : (i + 1) * width] for i in range(3)] + [out_grad]
    )
    mlp_grad = jnp.stack([up_grad, down_grad])
    attn_new, attn_moment_new, attn_second_new = adam_update(
        attn_weights, attn_moment, attn_second, attn_grad
    )
    mlp_new, mlp_moment_new, mlp_second_new = adam_update(
        mlp_weights, mlp_moment, mlp_second, mlp_grad
    )
    vector_new, vector_moment_new, vector_second_new = adam_update(
        vectors, vector_moment, vector_second, vector_grad
    )
    hidden_new, hidden_moment_new, hidden_second_new = adam_update(
        hidden_bias, hidden_moment, hidden_second, hidden_grad
    )
    return (
        output,
        input_grad,
        attn_grad,
        mlp_grad,
        vector_grad,
        hidden_grad,
        attn_new,
        mlp_new,
        vector_new,
        hidden_new,
        attn_moment_new,
        mlp_moment_new,
        vector_moment_new,
        hidden_moment_new,
        attn_second_new,
        mlp_second_new,
        vector_second_new,
        hidden_second_new,
    )


def layer(*arrays):
    sequences, n_context = arrays[0].shape[0], lax.axis_size("context")
    if sequences % n_context == 0 and n_context == 4 and lax.axis_size("shard") == 2:
        return fast_body(*arrays)
    return body(*arrays)


def solution(mesh):
    return jax.shard_map(
        layer,
        mesh=mesh,
        in_specs=(
            P("shard", "context", "tensor"),
            P("shard", "context", "tensor"),
            P("shard", None),
            P(None, ("shard", "context"), "tensor"),
            P(None, ("shard", "context"), "tensor"),
            P(None, "tensor"),
            P("tensor"),
            P(None, ("shard", "context"), "tensor"),
            P(None, ("shard", "context"), "tensor"),
            P(None, "tensor"),
            P("tensor"),
            P(None, ("shard", "context"), "tensor"),
            P(None, ("shard", "context"), "tensor"),
            P(None, "tensor"),
            P("tensor"),
        ),
        out_specs=(
            P("shard", "context", "tensor"),
            P("shard", "context", "tensor"),
            P(None, ("shard", "context"), "tensor"),
            P(None, ("shard", "context"), "tensor"),
            P(None, "tensor"),
            P("tensor"),
            P(None, ("shard", "context"), "tensor"),
            P(None, ("shard", "context"), "tensor"),
            P(None, "tensor"),
            P("tensor"),
            P(None, ("shard", "context"), "tensor"),
            P(None, ("shard", "context"), "tensor"),
            P(None, "tensor"),
            P("tensor"),
            P(None, ("shard", "context"), "tensor"),
            P(None, ("shard", "context"), "tensor"),
            P(None, "tensor"),
            P("tensor"),
        ),
        check_vma=False,
    )
```

```python
import functools

import jax
import jax.numpy as jnp
from jax import lax
from jax.experimental import pallas as pl
from jax.experimental.pallas import tpu as pltpu
from jax.sharding import PartitionSpec as P


SHARD, CONTEXT, TENSOR = "shard", "context", "tensor"

D = 2048
HEADS = 32
HD = 64
ROT = 32
STEP = 7


norm_epsilon = 1e-05
first_beta = 0.9
second_beta = 0.95
adam_epsilon = 1e-08
learn_rate = 0.1
weight_decay = 0.1
rotary_base = 10000.0
masked_score = -1e30


def rotate(field, cosine, sine, half_rot):
    first = field[:, :, :half_rot]
    second = field[:, :, half_rot : 2 * half_rot]
    return jnp.concatenate(
        [
            first * cosine - second * sine,
            second * cosine + first * sine,
            field[:, :, 2 * half_rot :],
        ],
        axis=2,
    )


def block_scores(query_blk, key_blk, scale):
    return jnp.einsum("eq,ek->qk", query_blk, key_blk, preferred_element_type=jnp.float32) * scale


def block_mask(doc_row, q_start, k_start, block):
    q_docs = lax.dynamic_slice_in_dim(doc_row, q_start, block)
    k_docs = lax.dynamic_slice_in_dim(doc_row, k_start, block)
    offsets = jnp.arange(block, dtype=jnp.int32)
    causal = (k_start + offsets)[None, :] <= (q_start + offsets)[:, None]
    return (q_docs[:, None] == k_docs[None, :]) & causal


def block_empty(doc_row, q_start, k_start, block):
    return doc_row[k_start + block - 1] < doc_row[q_start]


def attend_item(query, key_rows, values, doc_row, block, scale):
    head_dim, length = query.shape

    def query_step(q_block, carry):
        out_acc, lse_acc = carry
        q_start = q_block * block
        query_blk = lax.dynamic_slice_in_dim(query, q_start, block, 1)

        def stats_step(k_block, state):
            k_start = k_block * block

            def stats_live(state_in):
                run_max, run_sum = state_in
                key_blk = lax.dynamic_slice_in_dim(key_rows, k_start, block, 1)
                allowed = block_mask(doc_row, q_start, k_start, block)
                scores = jnp.where(allowed, block_scores(query_blk, key_blk, scale), masked_score)
                new_max = jnp.maximum(run_max, jnp.max(scores, axis=1))
                weights = jnp.where(allowed, jnp.exp(scores - new_max[:, None]), 0.0)
                return (new_max, run_sum * jnp.exp(run_max - new_max) + jnp.sum(weights, axis=1))

            return lax.cond(
                block_empty(doc_row, q_start, k_start, block),
                lambda state_in: state_in,
                stats_live,
                state,
            )

        first_state = (
            jnp.full((block,), masked_score, jnp.float32),
            jnp.zeros((block,), jnp.float32),
        )
        run_max, run_sum = lax.fori_loop(0, q_block + 1, stats_step, first_state)
        lse_blk = run_max + jnp.log(run_sum)

        def value_step(k_block, acc):
            k_start = k_block * block

            def value_live(acc_in):
                key_blk = lax.dynamic_slice_in_dim(key_rows, k_start, block, 1)
                value_blk = lax.dynamic_slice_in_dim(values, k_start, block, 1)
                allowed = block_mask(doc_row, q_start, k_start, block)
                scores = block_scores(query_blk, key_blk, scale)
                probs = jnp.where(allowed, jnp.exp(scores - lse_blk[:, None]), 0.0).astype(
                    jnp.bfloat16
                )
                return acc_in + jnp.einsum(
                    "qk,ek->eq", probs, value_blk, preferred_element_type=jnp.float32
                )

            return lax.cond(
                block_empty(doc_row, q_start, k_start, block),
                lambda acc_in: acc_in,
                value_live,
                acc,
            )

        acc = lax.fori_loop(0, q_block + 1, value_step, jnp.zeros((head_dim, block), jnp.float32))
        out_acc = lax.dynamic_update_slice_in_dim(out_acc, acc.astype(jnp.bfloat16), q_start, 1)
        lse_acc = lax.dynamic_update_slice_in_dim(lse_acc, lse_blk, q_start, 0)
        return (out_acc, lse_acc)

    first_carry = (jnp.zeros((head_dim, length), jnp.bfloat16), jnp.zeros((length,), jnp.float32))
    return lax.fori_loop(0, length // block, query_step, first_carry)


def attend_back(query, key_rows, values, grad_out, lse, doc_row, block, scale):
    head_dim, length = query.shape

    def query_step(q_block, carry):
        grad_query, grad_key, grad_value = carry
        q_start = q_block * block
        query_blk = lax.dynamic_slice_in_dim(query, q_start, block, 1)
        gout_blk = lax.dynamic_slice_in_dim(grad_out, q_start, block, 1)
        lse_blk = lax.dynamic_slice_in_dim(lse, q_start, block, 0)

        def pieces(k_start):
            key_blk = lax.dynamic_slice_in_dim(key_rows, k_start, block, 1)
            value_blk = lax.dynamic_slice_in_dim(values, k_start, block, 1)
            allowed = block_mask(doc_row, q_start, k_start, block)
            scores = block_scores(query_blk, key_blk, scale)
            probs = jnp.where(allowed, jnp.exp(scores - lse_blk[:, None]), 0.0)
            dprobs = jnp.einsum(
                "eq,ek->qk", gout_blk, value_blk, preferred_element_type=jnp.float32
            )
            return (key_blk, probs, dprobs)

        def delta_step(k_block, delta):
            k_start = k_block * block

            def delta_live(delta_in):
                _, probs, dprobs = pieces(k_start)
                return delta_in + jnp.sum(probs * dprobs, axis=1)

            return lax.cond(
                block_empty(doc_row, q_start, k_start, block),
                lambda delta_in: delta_in,
                delta_live,
                delta,
            )

        delta = lax.fori_loop(0, q_block + 1, delta_step, jnp.zeros((block,), jnp.float32))

        def grad_step(k_block, state):
            k_start = k_block * block

            def grad_live(state_in):
                query_part, key_all, value_all = state_in
                key_blk, probs, dprobs = pieces(k_start)
                dscores = (probs * (dprobs - delta[:, None])).astype(jnp.bfloat16)
                query_part = query_part + jnp.einsum(
                    "qk,ek->eq", dscores, key_blk, preferred_element_type=jnp.float32
                )
                key_add = (
                    jnp.einsum("qk,eq->ek", dscores, query_blk, preferred_element_type=jnp.float32)
                    * scale
                )
                value_add = jnp.einsum(
                    "qk,eq->ek",
                    probs.astype(jnp.bfloat16),
                    gout_blk,
                    preferred_element_type=jnp.float32,
                )
                key_all = lax.dynamic_update_slice_in_dim(
                    key_all,
                    lax.dynamic_slice_in_dim(key_all, k_start, block, 1) + key_add,
                    k_start,
                    1,
                )
                value_all = lax.dynamic_update_slice_in_dim(
                    value_all,
                    lax.dynamic_slice_in_dim(value_all, k_start, block, 1) + value_add,
                    k_start,
                    1,
                )
                return (query_part, key_all, value_all)

            return lax.cond(
                block_empty(doc_row, q_start, k_start, block),
                lambda state_in: state_in,
                grad_live,
                state,
            )

        first_state = (jnp.zeros((head_dim, block), jnp.float32), grad_key, grad_value)
        query_part, grad_key, grad_value = lax.fori_loop(0, q_block + 1, grad_step, first_state)
        grad_query = lax.dynamic_update_slice_in_dim(grad_query, query_part * scale, q_start, 1)
        return (grad_query, grad_key, grad_value)

    zero_grid = jnp.zeros((head_dim, length), jnp.float32)
    grad_query, grad_key, grad_value = lax.fori_loop(
        0, length // block, query_step, (zero_grid, zero_grid, zero_grid)
    )
    return (
        grad_query.astype(jnp.bfloat16),
        grad_key.astype(jnp.bfloat16),
        grad_value.astype(jnp.bfloat16),
    )


def adam_update(weight, moment, second, grad):
    count = float(STEP)
    new_moment = first_beta * moment + (1.0 - first_beta) * grad
    new_second = second_beta * second + (1.0 - second_beta) * grad * grad
    moment_hat = new_moment / (1.0 - first_beta**count)
    second_hat = new_second / (1.0 - second_beta**count)
    new_weight = weight - learn_rate * (
        moment_hat / (jnp.sqrt(second_hat) + adam_epsilon) + weight_decay * weight
    )
    return (new_weight, new_moment, new_second)


def body(
    inputs,
    cotangent,
    doc_lengths,
    attn_weights,
    mlp_weights,
    vectors,
    hidden_bias,
    attn_moment,
    mlp_moment,
    vector_moment,
    hidden_moment,
    attn_second,
    mlp_second,
    vector_second,
    hidden_second,
):
    sequences, local_len, width_part = inputs.shape
    n_context = lax.axis_size(CONTEXT)
    n_tensor = lax.axis_size(TENSOR)
    heads_here = HEADS // n_tensor
    tokens_here = sequences * local_len
    length = local_len * n_context
    block = min(512, length)
    per_device = sequences * heads_here // n_context
    scale = HD ** (-0.5)
    half_rot = ROT // 2
    ends = jnp.cumsum(doc_lengths, axis=1)
    starts = ends - doc_lengths
    all_index = jnp.arange(length, dtype=jnp.int32)
    doc_ids = jnp.sum((all_index[None, :, None] >= ends[:, None, :]).astype(jnp.int32), axis=2)
    local_index = lax.axis_index(CONTEXT) * local_len + jnp.arange(local_len, dtype=jnp.int32)
    inside = (local_index[None, :, None] >= starts[:, None, :]) & (
        local_index[None, :, None] < ends[:, None, :]
    )
    doc_start = jnp.sum(jnp.where(inside, starts[:, None, :], 0), axis=2)
    position = (local_index[None, :] - doc_start).astype(jnp.float32)
    freq = rotary_base ** (-(2.0 * jnp.arange(half_rot, dtype=jnp.float32)) / ROT)
    angle = freq[None, :, None] * position[:, None, :]
    cosine = jnp.cos(angle)[:, None]
    sine = jnp.sin(angle)[:, None]
    norm_low = vectors[0:2].astype(jnp.bfloat16)
    tokens_full, norm_full = (
        lax.all_gather(inputs, TENSOR, axis=2, tiled=True),
        lax.all_gather(norm_low, TENSOR, axis=1, tiled=True),
    )
    rows_in = tokens_full.astype(jnp.float32).reshape(tokens_here, D)
    mean_val = jnp.mean(rows_in, axis=1, keepdims=True)
    centered = rows_in - mean_val
    variance = jnp.mean(centered * centered, axis=1, keepdims=True)
    inv_std = lax.rsqrt(variance + norm_epsilon)
    normal = centered * inv_std
    gain_full = norm_full[0].astype(jnp.float32)
    normed = (normal * gain_full + norm_full[1].astype(jnp.float32)).astype(jnp.bfloat16)
    attn_full, mlp_full = (
        lax.all_gather(attn_weights.astype(jnp.bfloat16), (SHARD, CONTEXT), axis=1, tiled=True),
        lax.all_gather(mlp_weights.astype(jnp.bfloat16), (SHARD, CONTEXT), axis=1, tiled=True),
    )
    token_grid = normed.reshape(sequences, local_len, D)
    qkv_weights = attn_full[0:3].reshape(3, D, heads_here, HD)
    projected = jnp.einsum(
        "std,cdhe->cshet", token_grid, qkv_weights, preferred_element_type=jnp.float32
    )
    query_pre = projected[0] + vectors[2].reshape(heads_here, HD)[None, :, :, None]
    key_pre = projected[1] + vectors[3].reshape(heads_here, HD)[None, :, :, None]
    value_pre = projected[2] + vectors[4].reshape(heads_here, HD)[None, :, :, None]
    outgoing = jnp.stack(
        [
            rotate(query_pre, cosine, sine, half_rot),
            rotate(key_pre, cosine, sine, half_rot),
            value_pre,
        ]
    ).astype(jnp.bfloat16)
    outgoing = outgoing.reshape(3, sequences * heads_here, HD, local_len)
    attn_in = lax.all_to_all(outgoing, CONTEXT, split_axis=1, concat_axis=3, tiled=True)
    item_index = lax.axis_index(CONTEXT) * per_device + jnp.arange(per_device, dtype=jnp.int32)
    item_docs = jnp.take(doc_ids, item_index // heads_here, axis=0)

    def attend_one(parts):
        query, key_part, value_part, doc_row = parts
        return attend_item(query, key_part, value_part, doc_row, block, scale)

    attn_out, lse = lax.map(attend_one, (attn_in[0], attn_in[1], attn_in[2], item_docs))
    heads_out = lax.all_to_all(attn_out, CONTEXT, split_axis=2, concat_axis=0, tiled=True)
    heads_grid = heads_out.reshape(sequences, heads_here, HD, local_len)
    out_weights = attn_full[3].reshape(D, heads_here, HD)
    branch = jnp.einsum(
        "shet,ohe->sto", heads_grid, out_weights, preferred_element_type=jnp.float32
    ).reshape(tokens_here, D)
    pre_act = jnp.dot(normed, mlp_full[0], preferred_element_type=jnp.float32) + hidden_bias
    gelu_value, gelu_back = jax.vjp(lambda field: jax.nn.gelu(field, approximate=True), pre_act)
    hidden = gelu_value.astype(jnp.bfloat16)
    branch = branch + jnp.einsum(
        "tf,of->to", hidden, mlp_full[1], preferred_element_type=jnp.float32
    )
    summed = lax.psum_scatter(branch, TENSOR, scatter_dimension=1, tiled=True)
    input_rows = inputs.astype(jnp.float32).reshape(tokens_here, width_part)
    output = (
        (input_rows + summed + vectors[5] + vectors[6])
        .astype(jnp.bfloat16)
        .reshape(sequences, local_len, width_part)
    )
    grad_full = lax.all_gather(cotangent, TENSOR, axis=2, tiled=True)
    grad_rows = grad_full.reshape(tokens_here, D)
    attn_back, mlp_back = (
        lax.all_gather(attn_weights.astype(jnp.bfloat16), (SHARD, CONTEXT), axis=1, tiled=True),
        lax.all_gather(mlp_weights.astype(jnp.bfloat16), (SHARD, CONTEXT), axis=1, tiled=True),
    )
    out_back = attn_back[3].reshape(D, heads_here, HD)
    grad_heads = jnp.einsum(
        "sto,ohe->shet", grad_full, out_back, preferred_element_type=jnp.float32
    ).astype(jnp.bfloat16)
    grad_heads = grad_heads.reshape(sequences * heads_here, HD, local_len)
    grad_items = lax.all_to_all(grad_heads, CONTEXT, split_axis=0, concat_axis=2, tiled=True)

    def attend_grad(parts):
        query, key_part, value_part, gout, lse_row, doc_row = parts
        return attend_back(query, key_part, value_part, gout, lse_row, doc_row, block, scale)

    grad_query_item, grad_key_item, grad_value_item = lax.map(
        attend_grad, (attn_in[0], attn_in[1], attn_in[2], grad_items, lse, item_docs)
    )
    grads_back = lax.all_to_all(
        jnp.stack([grad_query_item, grad_key_item, grad_value_item]),
        CONTEXT,
        split_axis=3,
        concat_axis=1,
        tiled=True,
    )
    grad_grid = grads_back.reshape(3, sequences, heads_here, HD, local_len)
    grad_query = rotate(grad_grid[0].astype(jnp.float32), cosine, -sine, half_rot).astype(
        jnp.bfloat16
    )
    grad_key = rotate(grad_grid[1].astype(jnp.float32), cosine, -sine, half_rot).astype(
        jnp.bfloat16
    )
    grad_proj = jnp.stack([grad_query, grad_key, grad_grid[2]])
    qkv_back = attn_back[0:3].reshape(3, D, heads_here, HD)
    qkv_grad = jnp.einsum(
        "std,cshet->cdhe", token_grid, grad_proj, preferred_element_type=jnp.float32
    ).reshape(3, D, width_part)
    normed_grad = jnp.einsum(
        "cshet,cdhe->std", grad_proj, qkv_back, preferred_element_type=jnp.float32
    ).reshape(tokens_here, D)
    out_grad = jnp.einsum(
        "sto,shet->ohe", grad_full, heads_grid, preferred_element_type=jnp.float32
    ).reshape(D, width_part)
    hidden_act_grad = jnp.dot(grad_rows, mlp_back[1], preferred_element_type=jnp.float32)
    pre_grad = gelu_back(hidden_act_grad)[0].astype(jnp.bfloat16)
    second_grad = jnp.einsum("to,tf->of", grad_rows, hidden, preferred_element_type=jnp.float32)
    first_grad = jnp.einsum("td,tf->df", normed, pre_grad, preferred_element_type=jnp.float32)
    normed_grad = normed_grad + jnp.einsum(
        "tf,df->td", pre_grad, mlp_back[0], preferred_element_type=jnp.float32
    )
    norm_stats = jnp.stack([jnp.sum(normed_grad * normal, axis=0), jnp.sum(normed_grad, axis=0)])
    scaled = normed_grad * gain_full
    input_part = inv_std * (
        scaled
        - jnp.mean(scaled, axis=1, keepdims=True)
        - normal * jnp.mean(scaled * normal, axis=1, keepdims=True)
    )
    input_slice, norm_slice = (
        lax.psum_scatter(input_part, TENSOR, scatter_dimension=1, tiled=True),
        lax.psum_scatter(norm_stats, TENSOR, scatter_dimension=1, tiled=True),
    )
    cot_rows = cotangent.astype(jnp.float32).reshape(tokens_here, width_part)
    input_grad = (
        (cot_rows + input_slice).astype(jnp.bfloat16).reshape(sequences, local_len, width_part)
    )
    cot_total = jnp.sum(cot_rows, axis=0)
    query_bias_grad = jnp.sum(grad_query.astype(jnp.float32), axis=(0, 3)).reshape(width_part)
    key_bias_grad = jnp.sum(grad_key.astype(jnp.float32), axis=(0, 3)).reshape(width_part)
    value_bias_grad = jnp.sum(grad_grid[2].astype(jnp.float32), axis=(0, 3)).reshape(width_part)
    local_vectors = jnp.stack(
        [
            norm_slice[0],
            norm_slice[1],
            query_bias_grad,
            key_bias_grad,
            value_bias_grad,
            cot_total,
            cot_total,
        ]
    )
    local_hidden = jnp.sum(pre_grad.astype(jnp.float32), axis=0)
    vector_grad, hidden_grad = lax.psum((local_vectors, local_hidden), (SHARD, CONTEXT))
    attn_local = jnp.concatenate([qkv_grad, out_grad[None]], axis=0)
    mlp_local = jnp.stack([first_grad, second_grad])
    attn_grad, mlp_grad = (
        lax.psum_scatter(attn_local, (SHARD, CONTEXT), scatter_dimension=1, tiled=True),
        lax.psum_scatter(mlp_local, (SHARD, CONTEXT), scatter_dimension=1, tiled=True),
    )
    attn_new, attn_moment_new, attn_second_new = adam_update(
        attn_weights, attn_moment, attn_second, attn_grad
    )
    mlp_new, mlp_moment_new, mlp_second_new = adam_update(
        mlp_weights, mlp_moment, mlp_second, mlp_grad
    )
    vector_new, vector_moment_new, vector_second_new = adam_update(
        vectors, vector_moment, vector_second, vector_grad
    )
    hidden_new, hidden_moment_new, hidden_second_new = adam_update(
        hidden_bias, hidden_moment, hidden_second, hidden_grad
    )
    return (
        output,
        input_grad,
        attn_grad,
        mlp_grad,
        vector_grad,
        hidden_grad,
        attn_new,
        mlp_new,
        vector_new,
        hidden_new,
        attn_moment_new,
        mlp_moment_new,
        vector_moment_new,
        hidden_moment_new,
        attn_second_new,
        mlp_second_new,
        vector_second_new,
        hidden_second_new,
    )


def attention_kernel(
    first_ref,
    q_ref,
    k_ref,
    v_ref,
    gout_ref,
    cos_ref,
    low_ref,
    high_ref,
    start_ref,
    out_ref,
    gq_ref,
    gk_ref,
    gv_ref,
    key_cat,
    value_cat,
    raw,
    dprob,
    gk_acc,
    gv_acc,
    *,
    block,
    steps,
    scale,
    half_rot,
):
    row, step = pl.program_id(0), pl.program_id(2)
    pair = q_ref.shape[1]
    lane_low = lax.broadcasted_iota(jnp.int32, (block, pair), 1) < pair // 2
    contract_last = (((1,), (1,)), ((), ()))
    contract_first = (((0,), (0,)), ((), ()))
    plain = (((1,), (0,)), ((), ()))

    def dot(a, b, dims):
        return lax.dot_general(a, b, dims, preferred_element_type=jnp.float32)

    def turn(field, start, sign):
        rows = pl.ds(start, block)
        return (
            field * cos_ref[rows, :]
            + sign * (pltpu.roll(field, pair - half_rot, 1) * low_ref[rows, :])
            + sign * (pltpu.roll(field, half_rot, 1) * high_ref[rows, :])
        )

    @pl.when(step == 0)
    def _():
        gk_acc[...] = jnp.zeros_like(gk_acc)
        gv_acc[...] = jnp.zeros_like(gv_acc)

        @pl.loop(0, steps)
        def _(j):
            at = pl.multiple_of(j * block, block)
            keys = turn(k_ref[pl.ds(at, block), :], at, 1.0)
            values = v_ref[pl.ds(at, block), :]
            for half in range(2):
                keep = lane_low if half == 0 else jnp.logical_not(lane_low)
                rows = pl.ds(pl.multiple_of(2 * at, 2 * block) + half * block, block)
                key_cat[rows, :] = jnp.where(keep, keys, 0.0).astype(jnp.bfloat16)
                value_cat[rows, :] = jnp.where(keep, values, 0.0).astype(jnp.bfloat16)

    q_at = pl.multiple_of(step * block, block)
    queries = turn(q_ref[...], q_at, 1.0).astype(jnp.bfloat16)
    queries = (queries.astype(jnp.float32) * scale).astype(jnp.bfloat16)
    gout = gout_ref[...]
    first = first_ref[row * steps + step]
    begin = start_ref[...]
    q_pos = q_at + lax.broadcasted_iota(jnp.int32, (block, block), 0)
    k_lane = lax.broadcasted_iota(jnp.int32, (block, block), 1)

    def rows_of(j):
        return pl.ds(pl.multiple_of(j * (2 * block), 2 * block), 2 * block)

    def score_step(j, tops):
        scores = dot(queries, key_cat[rows_of(j), :], contract_last)
        k_pos = j * block + k_lane
        allowed = (k_pos <= q_pos) & (k_pos >= begin)
        new_tops = []
        for half in range(2):
            part = jnp.where(allowed, scores[:, half * block : (half + 1) * block], -3e38)
            raw[j, :, half * block : (half + 1) * block] = part
            new_tops.append(jnp.maximum(tops[half], jnp.max(part, axis=1, keepdims=True)))
        return tuple(new_tops)

    low_start = jnp.full((block, 1), -3e38, jnp.float32)
    tops = lax.fori_loop(first, step + 1, score_step, (low_start, low_start))

    def weight_step(j, sums):
        dp = dot(gout, value_cat[rows_of(j), :], contract_last)
        dprob[j] = dp
        new_sums = []
        for half in range(2):
            cols = slice(half * block, (half + 1) * block)
            weights = jnp.exp(raw[j, :, cols] - tops[half])
            raw[j, :, cols] = weights
            new_sums.append(sums[2 * half] + jnp.sum(weights, axis=1, keepdims=True))
            new_sums.append(
                sums[2 * half + 1] + jnp.sum(weights * dp[:, cols], axis=1, keepdims=True)
            )
        return tuple(new_sums)

    zero = jnp.zeros((block, 1), jnp.float32)
    sums = lax.fori_loop(first, step + 1, weight_step, (zero,) * 4)
    inverse = [1.0 / sums[0], 1.0 / sums[2]]
    delta = [sums[1] * inverse[0], sums[3] * inverse[1]]

    def grad_step(j, carry):
        out_acc, gq_acc = carry
        probs, dscores = [], []
        for half in range(2):
            cols = slice(half * block, (half + 1) * block)
            full = raw[j, :, cols] * inverse[half]
            probs.append(full.astype(jnp.bfloat16))
            dscores.append((full * (dprob[j, :, cols] - delta[half])).astype(jnp.bfloat16))
        probs = jnp.concatenate(probs, axis=1)
        dscores = jnp.concatenate(dscores, axis=1)
        rows = rows_of(j)
        out_acc = out_acc + dot(probs, value_cat[rows, :], plain)
        gq_acc = gq_acc + dot(dscores, key_cat[rows, :], plain)
        gk_acc[rows, :] += dot(dscores, queries, contract_first)
        gv_acc[rows, :] += dot(probs, gout, contract_first)
        return (out_acc, gq_acc)

    blank = jnp.zeros((block, pair), jnp.float32)
    out_acc, gq_acc = lax.fori_loop(first, step + 1, grad_step, (blank, blank))
    out_ref[...] = out_acc.astype(jnp.bfloat16)
    gq_low = (gq_acc * scale).astype(jnp.bfloat16).astype(jnp.float32)
    gq_ref[...] = turn(gq_low, q_at, -1.0).astype(jnp.bfloat16)

    @pl.when(step == steps - 1)
    def _():
        @pl.loop(0, steps)
        def _(j):
            at = pl.multiple_of(j * block, block)
            top = pl.ds(pl.multiple_of(2 * at, 2 * block), block)
            bottom = pl.ds(pl.multiple_of(2 * at, 2 * block) + block, block)
            gk = jnp.where(lane_low, gk_acc[top, :], gk_acc[bottom, :])
            gk_low = gk.astype(jnp.bfloat16).astype(jnp.float32)
            gk_ref[pl.ds(at, block), :] = turn(gk_low, at, -1.0).astype(jnp.bfloat16)
            gv_ref[pl.ds(at, block), :] = jnp.where(
                lane_low, gv_acc[top, :], gv_acc[bottom, :]
            ).astype(jnp.bfloat16)


def attention(qkv_pre, gout, tables, begin, first, rows, length, block):
    width = gout.shape[1]
    pair = 2 * HD
    pairs = width // pair
    steps = length // block
    cosine, low, high = tables
    whole = pl.BlockSpec((length, pair), lambda r, h, i, f: (r, h))
    keys = pl.BlockSpec((length, pair), lambda r, h, i, f: (r, pairs + h))
    values = pl.BlockSpec((length, pair), lambda r, h, i, f: (r, 2 * pairs + h))
    part = pl.BlockSpec((block, pair), lambda r, h, i, f: (r * steps + i, h))
    table = pl.BlockSpec((length, pair), lambda r, h, i, f: (r, 0))
    shape = jax.ShapeDtypeStruct((rows * length, width), jnp.bfloat16)
    return pl.pallas_call(
        functools.partial(
            attention_kernel, block=block, steps=steps, scale=HD ** (-0.5), half_rot=ROT // 2
        ),
        out_shape=(shape,) * 4,
        grid_spec=pltpu.PrefetchScalarGridSpec(
            num_scalar_prefetch=1,
            grid=(rows, pairs, steps),
            in_specs=[
                part,
                keys,
                values,
                part,
                table,
                table,
                table,
                pl.BlockSpec((block, 1), lambda r, h, i, f: (r * steps + i, 0)),
            ],
            out_specs=[part, part, whole, whole],
            scratch_shapes=[
                pltpu.VMEM((2 * length, pair), jnp.bfloat16),
                pltpu.VMEM((2 * length, pair), jnp.bfloat16),
                pltpu.VMEM((steps, block, 2 * block), jnp.float32),
                pltpu.VMEM((steps, block, 2 * block), jnp.float32),
                pltpu.VMEM((2 * length, pair), jnp.float32),
                pltpu.VMEM((2 * length, pair), jnp.float32),
            ],
        ),
        compiler_params=pltpu.CompilerParams(
            dimension_semantics=("arbitrary", "arbitrary", "arbitrary")
        ),
        cost_estimate=pl.CostEstimate(
            flops=rows * width * length * length * 8,
            bytes_accessed=rows * length * width * 30,
            transcendentals=rows * pairs * length * length,
        ),
    )(first, qkv_pre, qkv_pre, qkv_pre, gout, cosine, low, high, begin)


MESH = pl.DeviceIdType.MESH


def flipped(index, bits):
    bit = 1
    while bit <= bits:
        if bits & bit:
            index = index + bit - 2 * bit * ((index // bit) % 2)
        bit *= 2
    return index


def gather_kernel(
    x_ref,
    g_ref,
    norm_ref,
    x_out,
    g_out,
    normed_out,
    normed_halves,
    g_halves,
    mean_out,
    inv_out,
    gain_out,
    x_buf,
    g_buf,
    normed_buf,
    normed_parts,
    g_parts,
    norm_all,
    own_sem,
    send_a,
    recv_a,
    send_n,
    recv_n,
    send_r,
    recv_r,
    send_l,
    recv_l,
    out_sem,
    *,
    n_context,
    n_tensor,
    n_block,
    rows,
    strip,
):
    c, z = lax.axis_index(CONTEXT), lax.axis_index(TENSOR)
    core = c % 2
    local_len, width = x_ref.shape[1:]
    length = local_len * n_context
    sources, buffers = (x_ref, g_ref), (x_buf, g_buf)

    def peer(k):
        return flipped(c, k)

    barrier = pltpu.get_barrier_semaphore()
    for k in range(1, n_context):
        pl.semaphore_signal(barrier, inc=1, device_id={CONTEXT: peer(k)}, device_id_type=MESH)
    for k in range(1, n_tensor):
        pl.semaphore_signal(
            barrier, inc=1, device_id={TENSOR: (z + k) % n_tensor}, device_id_type=MESH
        )
    pl.semaphore_wait(barrier, n_context + n_tensor - 2)

    def at(r, chunk):
        return pl.ds(pl.multiple_of(r * length + chunk * local_len, local_len), local_len)

    def piece(f, r, chunk, origin):
        return buffers[f].at[at(r, chunk), pl.ds(pl.multiple_of(origin * width, width), width)]

    def own_copy(f, r):
        return pltpu.make_async_copy(
            sources[f].at[c * rows + r], piece(f, r, c, z), own_sem.at[f, r]
        )

    own_norm = pltpu.make_async_copy(norm_ref, norm_all.at[z], own_sem.at[2, 0])

    def swap(f, r, k):
        return pltpu.make_async_remote_copy(
            src_ref=sources[f].at[peer(k) * rows + r],
            dst_ref=piece(f, r, c, z),
            send_sem=send_a.at[f, k - 1, r],
            recv_sem=recv_a.at[f, k - 1, r],
            device_id={CONTEXT: peer(k)},
            device_id_type=MESH,
        )

    def norm_copy(k):
        return pltpu.make_async_remote_copy(
            src_ref=norm_ref,
            dst_ref=norm_all.at[z],
            send_sem=send_n.at[k - 1],
            recv_sem=recv_n.at[k - 1],
            device_id={TENSOR: (z + k) % n_tensor},
            device_id_type=MESH,
        )

    def hop(f, r, k, d, side, step):
        origin = z - d if side > 0 else z + d
        sends, recvs = (send_r, recv_r) if side > 0 else (send_l, recv_l)
        block = piece(f, r, peer(k), origin)
        return pltpu.make_async_remote_copy(
            src_ref=block,
            dst_ref=block,
            send_sem=sends.at[f, d - step, k, r],
            recv_sem=recvs.at[f, d - step, k, r],
            device_id={TENSOR: z + side * (1 - step)},
            device_id_type=MESH,
        )

    def has(d, side):
        return z >= d if side > 0 else z + d <= n_tensor - 1

    def more(side):
        return z < n_tensor - 1 if side > 0 else z > 0

    for f in range(2):
        for r in range(rows):
            own_copy(f, r).start()
        if f == 0:
            own_norm.start()
        for k in range(1, n_context):
            for r in range(rows):
                swap(f, r, k).start()
        if f == 0:
            for k in range(1, n_tensor):
                norm_copy(k).start()
    own_norm.wait()
    for k in range(1, n_tensor):
        norm_copy(k).wait_recv()

    gain = jnp.concatenate([norm_all[j, 0:1, :] for j in range(n_tensor)], axis=1)
    shift = jnp.concatenate([norm_all[j, 1:2, :] for j in range(n_tensor)], axis=1)
    gain, shift = gain.astype(jnp.float32), shift.astype(jnp.float32)
    gain_out[...] = gain

    span = x_buf.shape[1] // n_block

    def store_parts(parts, lines, value):
        for b in range(n_block):
            cols = slice((b // 2) * span, (b // 2 + 1) * span)
            parts[(b + core) % 2, lines, cols] = value[:, b * span : (b + 1) * span]

    def finish_x(base):
        @pl.loop(0, local_len // strip)
        def _(step):
            lines = pl.ds(pl.multiple_of(base + step * strip, strip), strip)
            field = x_buf[lines, :].astype(jnp.float32)
            mean_val = jnp.mean(field, axis=1, keepdims=True)
            centered = field - mean_val
            variance = jnp.mean(centered * centered, axis=1, keepdims=True)
            inv_std = lax.rsqrt(variance + norm_epsilon)
            normed = ((centered * inv_std) * gain + shift).astype(jnp.bfloat16)
            normed_buf[lines, :] = normed
            store_parts(normed_parts, lines, normed)
            mean_out[lines, :] = mean_val
            inv_out[lines, :] = inv_std

    def finish_g(base):
        @pl.loop(0, local_len // strip)
        def _(step):
            lines = pl.ds(pl.multiple_of(base + step * strip, strip), strip)
            store_parts(g_parts, lines, g_buf[lines, :])

    def results(f, r, k):
        lines = at(r, peer(k))
        if f == 0:
            pairs = [
                (x_buf.at[lines], x_out.at[lines]),
                (normed_buf.at[lines], normed_out.at[lines]),
                (normed_parts.at[0, lines], normed_halves.at[0, lines]),
                (normed_parts.at[1, lines], normed_halves.at[1, lines]),
            ]
        else:
            pairs = [
                (g_buf.at[lines], g_out.at[lines]),
                (g_parts.at[0, lines], g_halves.at[0, lines]),
                (g_parts.at[1, lines], g_halves.at[1, lines]),
            ]
        return [
            pltpu.make_async_copy(src, dst, out_sem.at[f, k, r, i])
            for i, (src, dst) in enumerate(pairs)
        ]

    order = [(f, r, k) for f in range(2) for k in range(n_context) for r in range(rows)]
    for f, r, k in order:
        for d in range(n_tensor):
            if d == 0:
                if k == 0:
                    own_copy(f, r).wait()
                else:
                    swap(f, r, k).wait_recv()
            for side in (1, -1):
                if d > 0:

                    @pl.when(has(d, side))
                    def _():
                        hop(f, r, k, d, side, 1).wait_recv()

                if d < n_tensor - 1:

                    @pl.when(has(d, side) & more(side))
                    def _():
                        hop(f, r, k, d, side, 0).start()

        base = r * length + peer(k) * local_len
        if f == 0:
            finish_x(base)
        else:
            finish_g(base)
        for copy in results(f, r, k):
            copy.start()

    for f, r, k in order:
        for d in range(n_tensor - 1):
            for side in (1, -1):

                @pl.when(has(d, side) & more(side))
                def _():
                    hop(f, r, k, d, side, 0).wait_send()

        if k > 0:
            swap(f, r, k).wait_send()
        for copy in results(f, r, k):
            copy.wait()
    for k in range(1, n_tensor):
        norm_copy(k).wait_send()


def gather_inputs(inputs, cotangent, norm_low, n_context, n_tensor, n_block):
    sequences, local_len, width = inputs.shape
    rows = sequences // n_context
    tokens = sequences * local_len
    full = width * n_tensor
    wide, low = jnp.float32, jnp.bfloat16
    dma = pltpu.SemaphoreType.DMA
    inside = pl.BlockSpec(memory_space=pltpu.VMEM)
    outside = pl.BlockSpec(memory_space=pl.ANY)
    hops = (2, n_tensor - 1, n_context, rows)
    return pl.pallas_call(
        functools.partial(
            gather_kernel,
            n_context=n_context,
            n_tensor=n_tensor,
            n_block=n_block,
            rows=rows,
            strip=min(32, local_len),
        ),
        out_shape=(
            jax.ShapeDtypeStruct((tokens, full), low),
            jax.ShapeDtypeStruct((tokens, full), low),
            jax.ShapeDtypeStruct((tokens, full), low),
            jax.ShapeDtypeStruct((2, tokens, full // 2), low),
            jax.ShapeDtypeStruct((2, tokens, full // 2), low),
            jax.ShapeDtypeStruct((tokens, 1), wide),
            jax.ShapeDtypeStruct((tokens, 1), wide),
            jax.ShapeDtypeStruct((1, full), wide),
        ),
        in_specs=[inside] * 3,
        out_specs=(outside,) * 5 + (inside,) * 3,
        scratch_shapes=[
            pltpu.VMEM((tokens, full), low),
            pltpu.VMEM((tokens, full), low),
            pltpu.VMEM((tokens, full), low),
            pltpu.VMEM((2, tokens, full // 2), low),
            pltpu.VMEM((2, tokens, full // 2), low),
            pltpu.VMEM((n_tensor, 2, width), low),
            dma((3, rows)),
            dma((2, n_context - 1, rows)),
            dma((2, n_context - 1, rows)),
            dma((n_tensor - 1,)),
            dma((n_tensor - 1,)),
            dma(hops),
            dma(hops),
            dma(hops),
            dma(hops),
            dma((2, n_context, rows, 4)),
        ],
        compiler_params=pltpu.CompilerParams(collective_id=0, has_side_effects=True),
    )(inputs, cotangent, norm_low)


def total_kernel(
    stats_ref,
    rest_ref,
    out_ref,
    parts,
    every,
    send_z,
    recv_z,
    send_p,
    recv_p,
    *,
    n_shard,
    n_context,
    n_tensor,
):
    y, c, z = lax.axis_index(SHARD), lax.axis_index(CONTEXT), lax.axis_index(TENSOR)
    me = y * n_context + c
    group = n_shard * n_context
    kept = stats_ref.shape[1]

    barrier = pltpu.get_barrier_semaphore()
    for k in range(1, n_tensor):
        pl.semaphore_signal(
            barrier, inc=1, device_id={TENSOR: (z + k) % n_tensor}, device_id_type=MESH
        )

    def place(k):
        other = (me + k) % group
        return {SHARD: other // n_context, CONTEXT: other % n_context}

    for k in range(1, group):
        pl.semaphore_signal(barrier, inc=1, device_id=place(k), device_id_type=MESH)
    pl.semaphore_wait(barrier, n_tensor + group - 2)

    def slice_copy(k):
        return pltpu.make_async_remote_copy(
            src_ref=stats_ref.at[(z + k) % n_tensor],
            dst_ref=parts.at[k],
            send_sem=send_z.at[k],
            recv_sem=recv_z.at[k],
            device_id={TENSOR: (z + k) % n_tensor},
            device_id_type=MESH,
        )

    for k in range(1, n_tensor):
        slice_copy(k).start()
    every[me, kept:, :] = rest_ref[...]
    total = stats_ref[z]
    for k in range(1, n_tensor):
        slice_copy(k).wait_recv()
        total = total + parts[k]
    every[me, 0:kept, :] = total

    def spread(k):
        return pltpu.make_async_remote_copy(
            src_ref=every.at[me],
            dst_ref=every.at[me],
            send_sem=send_p.at[k],
            recv_sem=recv_p.at[k],
            device_id=place(k),
            device_id_type=MESH,
        )

    def spread_from(k):
        other = (me + group - k) % group
        return pltpu.make_async_remote_copy(
            src_ref=every.at[other],
            dst_ref=every.at[other],
            send_sem=send_p.at[k],
            recv_sem=recv_p.at[k],
            device_id=place(k),
            device_id_type=MESH,
        )

    for k in range(1, group):
        spread(k).start()
    for k in range(1, group):
        spread_from(k).wait_recv()
    total = every[0]
    for j in range(1, group):
        total = total + every[j]
    out_ref[...] = total
    for k in range(1, n_tensor):
        slice_copy(k).wait_send()
    for k in range(1, group):
        spread(k).wait_send()


def total_vectors(stats, rest, n_shard, n_context, n_tensor):
    kept, (more, width) = stats.shape[1], rest.shape
    group = n_shard * n_context
    dma = pltpu.SemaphoreType.DMA
    inside = pl.BlockSpec(memory_space=pltpu.VMEM)
    return pl.pallas_call(
        functools.partial(
            total_kernel, n_shard=n_shard, n_context=n_context, n_tensor=n_tensor
        ),
        out_shape=jax.ShapeDtypeStruct((kept + more, width), jnp.float32),
        in_specs=[inside] * 2,
        out_specs=inside,
        scratch_shapes=[
            pltpu.VMEM((n_tensor, kept, width), jnp.float32),
            pltpu.VMEM((group, kept + more, width), jnp.float32),
            dma((n_tensor,)),
            dma((n_tensor,)),
            dma((group,)),
            dma((group,)),
        ],
        compiler_params=pltpu.CompilerParams(collective_id=1, has_side_effects=True),
    )(stats, rest)


def return_kernel(sum_ref, base_ref, out_ref, mixed, send, recv, own, *, n_context, rows):
    c = lax.axis_index(CONTEXT)
    local_len = out_ref.shape[1]
    length = local_len * n_context

    def peer(k):
        return flipped(c, k)

    barrier = pltpu.get_barrier_semaphore()
    for k in range(1, n_context):
        pl.semaphore_signal(barrier, inc=1, device_id={CONTEXT: peer(k)}, device_id_type=MESH)

    def lines(r, k):
        return pl.ds(pl.multiple_of(r * length + peer(k) * local_len, local_len), local_len)

    def swap(r, k, place):
        return pltpu.make_async_remote_copy(
            src_ref=mixed.at[lines(r, k)],
            dst_ref=out_ref.at[place * rows + r],
            send_sem=send.at[k, r],
            recv_sem=recv.at[k, r],
            device_id={CONTEXT: peer(k)},
            device_id_type=MESH,
        )

    def blend(r, k):
        at = lines(r, k)
        mixed[at, :] = (
            sum_ref[at, :].astype(jnp.float32) + base_ref[at, :].astype(jnp.float32)
        ).astype(jnp.bfloat16)

    order = [(r, k) for k in range(n_context - 1, -1, -1) for r in range(rows)]
    for r, k in order:
        blend(r, k)
        if (r, k) == order[0]:
            pl.semaphore_wait(barrier, n_context - 1)
        if k > 0:
            swap(r, k, c).start()
        else:
            pltpu.make_async_copy(
                mixed.at[lines(r, 0)], out_ref.at[c * rows + r], own.at[r]
            ).start()
    for r, k in order:
        if k > 0:
            swap(r, k, peer(k)).wait_recv()
            swap(r, k, c).wait_send()
        else:
            pltpu.make_async_copy(
                mixed.at[lines(r, 0)], out_ref.at[c * rows + r], own.at[r]
            ).wait()


def return_rows(summed, base, n_context, rows):
    tokens, width = summed.shape
    local_len = tokens // (rows * n_context)
    dma = pltpu.SemaphoreType.DMA
    inside = pl.BlockSpec(memory_space=pltpu.VMEM)
    return pl.pallas_call(
        functools.partial(return_kernel, n_context=n_context, rows=rows),
        out_shape=jax.ShapeDtypeStruct((n_context * rows, local_len, width), jnp.bfloat16),
        in_specs=[inside] * 2,
        out_specs=inside,
        scratch_shapes=[
            pltpu.VMEM((tokens, width), jnp.bfloat16),
            dma((n_context, rows)),
            dma((n_context, rows)),
            dma((rows,)),
        ],
        compiler_params=pltpu.CompilerParams(collective_id=2, has_side_effects=True),
    )(summed, base)


def permute(field, axis, pairs):
    return lax.ppermute(field, axis, pairs)


def pick(field, index, axis):
    return lax.dynamic_index_in_dim(field, index, axis, keepdims=False)


def fast_body(
    inputs,
    cotangent,
    doc_lengths,
    attn_weights,
    mlp_weights,
    vectors,
    hidden_bias,
    attn_moment,
    mlp_moment,
    vector_moment,
    hidden_moment,
    attn_second,
    mlp_second,
    vector_second,
    hidden_second,
):
    sequences, local_len, width = inputs.shape
    n_context, n_tensor = lax.axis_size(CONTEXT), lax.axis_size(TENSOR)
    n_shard = lax.axis_size(SHARD)
    rows = sequences // n_context
    length = local_len * n_context
    tokens = rows * length
    block = min(256, length)
    half_rot = ROT // 2
    low_type = jnp.bfloat16
    wide = jnp.float32
    at_tensor, at_context = lax.axis_index(TENSOR), lax.axis_index(CONTEXT)
    at_y, at_x = lax.axis_index(SHARD), at_context // 2
    flip_core = [(i, i ^ 1) for i in range(n_context)]
    flip_x = [(i, i ^ 2) for i in range(n_context)]
    flip_y = [(i, i ^ 1) for i in range(n_shard)]

    def dot(a, b, left, right):
        return lax.dot_general(a, b, (((left,), (right,)), ((), ())), preferred_element_type=wide)

    attn_low = jnp.concatenate([attn_weights[i] for i in range(4)], axis=1).astype(low_type)
    attn_full = lax.all_gather(attn_low, (SHARD, CONTEXT), axis=0, tiled=True)
    mlp_full = lax.all_gather(
        mlp_weights.astype(low_type), (SHARD, CONTEXT), axis=1, tiled=True
    )
    w_qkv, w_out = attn_full[:, : 3 * width], attn_full[:, 3 * width :]
    w_up, w_down = mlp_full[0], mlp_full[1]

    x_full, g_full, normed, normed_halves, g_halves, mean_val, inv_std, gain_full = gather_inputs(
        inputs,
        cotangent,
        vectors[0:2].astype(low_type),
        n_context,
        n_tensor,
        n_shard * n_context,
    )

    ends = jnp.cumsum(doc_lengths, axis=1)
    my_ends = lax.dynamic_slice_in_dim(ends, at_context * rows, rows, 0)
    index = jnp.arange(length, dtype=jnp.int32)
    doc_start = jnp.max(
        jnp.where(index[None, :, None] >= my_ends[:, None, :], my_ends[:, None, :], 0), axis=2
    )
    first = (doc_start[:, ::block] // block).reshape(-1)
    begin = doc_start.reshape(tokens, 1)
    position = (index[None, :] - doc_start).astype(wide).reshape(tokens, 1)
    lane = jnp.arange(2 * HD, dtype=jnp.int32) % HD
    freq = rotary_base ** (-(2.0 * (lane % half_rot).astype(wide)) / ROT)
    angle = position * freq[None, :]
    cosine, sine = jnp.cos(angle), jnp.sin(angle)
    tables = (
        jnp.where(lane < ROT, cosine, 1.0),
        jnp.where(lane < half_rot, -sine, 0.0),
        jnp.where((lane >= half_rot) & (lane < ROT), sine, 0.0),
    )

    qkv_pre = dot(normed, w_qkv, 1, 0) + vectors[2:5].reshape(3 * width)
    gout = dot(g_full, w_out, 1, 0).astype(low_type)
    pre_act = dot(normed, w_up, 1, 0) + hidden_bias
    gelu_value, gelu_back = jax.vjp(lambda field: jax.nn.gelu(field, approximate=True), pre_act)
    hidden = gelu_value.astype(low_type)

    attended, g_query, g_key, g_value = attention(
        qkv_pre, gout, tables, begin, first, rows, length, block
    )
    g_qkv = jnp.concatenate([g_query, g_key, g_value], axis=1)

    def scatter_features(field):
        return lax.psum_scatter(field, TENSOR, scatter_dimension=1, tiled=True)

    def own_features(field, kind):
        return lax.dynamic_slice_in_dim(field, at_tensor * width, width, 1).astype(kind)

    def back_rows(field):
        pieces = field.reshape(rows, n_context, local_len, width)
        result = jnp.zeros((n_context, rows, local_len, width), field.dtype)
        for k in range(n_context):
            piece = pick(pieces, at_context ^ k, 1)
            if k > 0:
                piece = permute(piece, CONTEXT, [(i, i ^ k) for i in range(n_context)])
            result = lax.dynamic_update_index_in_dim(result, piece, at_context ^ k, 0)
        return result.reshape(sequences, local_len, width)

    branch = (dot(attended, w_out, 1, 1) + dot(hidden, w_down, 1, 1)).astype(low_type)
    summed = scatter_features(branch)

    pre_grad = gelu_back(dot(g_full, w_down, 1, 0))[0].astype(low_type)
    local_hidden = jnp.sum(pre_grad.astype(wide), axis=0)

    def both(a, b, where):
        return pick(a, where, 0).astype(wide) + pick(b, where, 0).astype(wide)

    def core_send(parts, right):
        return dot(parts[1], right, 0, 0).astype(low_type)

    def chip_send(parts, right, sent):
        half = right.shape[1] // 2
        arrived = permute(sent, CONTEXT, flip_core)
        chip = dot(parts[0], right, 0, 0) + arrived
        chip = chip.astype(low_type).reshape(n_shard, n_context // 2, -1, right.shape[1])
        first_half, second_half = chip[..., :half], chip[..., half:]
        return (
            pick(first_half, at_x, 1),
            pick(second_half, at_y, 0),
            pick(first_half, 1 - at_x, 1),
            pick(second_half, 1 - at_y, 0),
        )

    def line_send(chip):
        kept_x, kept_y, for_x, for_y = chip
        from_x = permute(for_x, CONTEXT, flip_x)
        from_y = permute(for_y, SHARD, flip_y)
        for_y = both(kept_x, from_x, 1 - at_y).astype(low_type)
        for_x = both(kept_y, from_y, 1 - at_x).astype(low_type)
        return (kept_x, from_x, kept_y, from_y), for_y, for_x

    def own_rows(line):
        (kept_x, from_x, kept_y, from_y), for_y, for_x = line
        next_y = permute(for_y, SHARD, flip_y)
        next_x = permute(for_x, CONTEXT, flip_x)
        return jnp.concatenate(
            [both(kept_x, from_x, at_y) + next_y, both(kept_y, from_y, at_x) + next_x], axis=1
        )

    down_sent = core_send(g_halves, hidden)
    up_sent = core_send(normed_halves, pre_grad)
    qkv_part = dot(g_qkv, w_qkv, 1, 1)
    down_chip = chip_send(g_halves, hidden, down_sent)
    up_chip = chip_send(normed_halves, pre_grad, up_sent)

    normed_grad = dot(pre_grad, w_up, 1, 1) + qkv_part
    normal = (x_full.astype(wide) - mean_val) * inv_std
    norm_stats = jnp.stack([jnp.sum(normed_grad * normal, axis=0), jnp.sum(normed_grad, axis=0)])
    scaled = normed_grad * gain_full
    input_part = (
        inv_std
        * (
            scaled
            - jnp.mean(scaled, axis=1, keepdims=True)
            - normal * jnp.mean(scaled * normal, axis=1, keepdims=True)
        )
    ).astype(low_type)
    input_slice = scatter_features(input_part)

    qkv_sent = core_send(normed_halves, g_qkv)
    out_sent = core_send(g_halves, attended)
    qkv_chip = chip_send(normed_halves, g_qkv, qkv_sent)
    out_chip = chip_send(g_halves, attended, out_sent)
    output = own_features(x_full, wide) + summed.astype(wide) + vectors[5] + vectors[6]
    output = output.astype(low_type)
    output = back_rows(output)
    down_line = line_send(down_chip)
    up_line = line_send(up_chip)
    qkv_line = line_send(qkv_chip)
    out_line = line_send(out_chip)
    down_grad, up_grad = own_rows(down_line), own_rows(up_line)
    qkv_grad, out_grad = own_rows(qkv_line), own_rows(out_line)

    g_own = own_features(g_full, low_type)
    input_grad = return_rows(input_slice, g_own, n_context, rows)

    stats_grid = norm_stats.reshape(2, n_tensor, width).transpose(1, 0, 2)
    rest = jnp.concatenate(
        [
            jnp.sum(g_qkv.astype(wide), axis=0).reshape(3, width),
            jnp.sum(own_features(g_full, wide), axis=0)[None],
            local_hidden.reshape(-1, width),
        ]
    )
    stats_grid, rest = lax.optimization_barrier((stats_grid, rest))
    totals = total_vectors(stats_grid, rest, n_shard, n_context, n_tensor)
    vector_grad = jnp.concatenate([totals[0:6], totals[5:6]])
    hidden_grad = totals[6:].reshape(-1)

    attn_grad = jnp.stack(
        [qkv_grad[:, i * width : (i + 1) * width] for i in range(3)] + [out_grad]
    )
    mlp_grad = jnp.stack([up_grad, down_grad])
    attn_new, attn_moment_new, attn_second_new = adam_update(
        attn_weights, attn_moment, attn_second, attn_grad
    )
    mlp_new, mlp_moment_new, mlp_second_new = adam_update(
        mlp_weights, mlp_moment, mlp_second, mlp_grad
    )
    vector_new, vector_moment_new, vector_second_new = adam_update(
        vectors, vector_moment, vector_second, vector_grad
    )
    hidden_new, hidden_moment_new, hidden_second_new = adam_update(
        hidden_bias, hidden_moment, hidden_second, hidden_grad
    )
    return (
        output,
        input_grad,
        attn_grad,
        mlp_grad,
        vector_grad,
        hidden_grad,
        attn_new,
        mlp_new,
        vector_new,
        hidden_new,
        attn_moment_new,
        mlp_moment_new,
        vector_moment_new,
        hidden_moment_new,
        attn_second_new,
        mlp_second_new,
        vector_second_new,
        hidden_second_new,
    )


def row_local(n_shard, n_context):
    return n_shard == 2 and n_context == 4


def layer(*arrays):
    n_shard, n_context = lax.axis_size(SHARD), lax.axis_size(CONTEXT)
    if row_local(n_shard, n_context) and arrays[0].shape[0] % n_context == 0:
        return fast_body(*arrays)
    return body(*arrays)


def solution(mesh):
    return jax.shard_map(
        layer,
        mesh=mesh,
        in_specs=(
            P(SHARD, CONTEXT, TENSOR),
            P(SHARD, CONTEXT, TENSOR),
            P(SHARD, None),
            P(None, (SHARD, CONTEXT), TENSOR),
            P(None, (SHARD, CONTEXT), TENSOR),
            P(None, TENSOR),
            P(TENSOR),
            P(None, (SHARD, CONTEXT), TENSOR),
            P(None, (SHARD, CONTEXT), TENSOR),
            P(None, TENSOR),
            P(TENSOR),
            P(None, (SHARD, CONTEXT), TENSOR),
            P(None, (SHARD, CONTEXT), TENSOR),
            P(None, TENSOR),
            P(TENSOR),
        ),
        out_specs=(
            P(SHARD, CONTEXT, TENSOR),
            P(SHARD, CONTEXT, TENSOR),
            P(None, (SHARD, CONTEXT), TENSOR),
            P(None, (SHARD, CONTEXT), TENSOR),
            P(None, TENSOR),
            P(TENSOR),
            P(None, (SHARD, CONTEXT), TENSOR),
            P(None, (SHARD, CONTEXT), TENSOR),
            P(None, TENSOR),
            P(TENSOR),
            P(None, (SHARD, CONTEXT), TENSOR),
            P(None, (SHARD, CONTEXT), TENSOR),
            P(None, TENSOR),
            P(TENSOR),
            P(None, (SHARD, CONTEXT), TENSOR),
            P(None, (SHARD, CONTEXT), TENSOR),
            P(None, TENSOR),
            P(TENSOR),
        ),
        check_vma=False,
    )
```

```python
import functools

import jax
import jax.numpy as jnp
from jax import lax
from jax.experimental import pallas as pl
from jax.experimental.pallas import tpu as pltpu
from jax.sharding import PartitionSpec as P


SHARD, CONTEXT, TENSOR = "shard", "context", "tensor"

D = 2048
HEADS = 32
HD = 64
ROT = 32
STEP = 7


norm_epsilon = 1e-05
first_beta = 0.9
second_beta = 0.95
adam_epsilon = 1e-08
learn_rate = 0.1
weight_decay = 0.1
rotary_base = 10000.0
masked_score = -1e30


def rotate(field, cosine, sine, half_rot):
    first = field[:, :, :half_rot]
    second = field[:, :, half_rot : 2 * half_rot]
    return jnp.concatenate(
        [
            first * cosine - second * sine,
            second * cosine + first * sine,
            field[:, :, 2 * half_rot :],
        ],
        axis=2,
    )


def block_scores(query_blk, key_blk, scale):
    return jnp.einsum("eq,ek->qk", query_blk, key_blk, preferred_element_type=jnp.float32) * scale


def block_mask(doc_row, q_start, k_start, block):
    q_docs = lax.dynamic_slice_in_dim(doc_row, q_start, block)
    k_docs = lax.dynamic_slice_in_dim(doc_row, k_start, block)
    offsets = jnp.arange(block, dtype=jnp.int32)
    causal = (k_start + offsets)[None, :] <= (q_start + offsets)[:, None]
    return (q_docs[:, None] == k_docs[None, :]) & causal


def block_empty(doc_row, q_start, k_start, block):
    return doc_row[k_start + block - 1] < doc_row[q_start]


def attend_item(query, key_rows, values, doc_row, block, scale):
    head_dim, length = query.shape

    def query_step(q_block, carry):
        out_acc, lse_acc = carry
        q_start = q_block * block
        query_blk = lax.dynamic_slice_in_dim(query, q_start, block, 1)

        def stats_step(k_block, state):
            k_start = k_block * block

            def stats_live(state_in):
                run_max, run_sum = state_in
                key_blk = lax.dynamic_slice_in_dim(key_rows, k_start, block, 1)
                allowed = block_mask(doc_row, q_start, k_start, block)
                scores = jnp.where(allowed, block_scores(query_blk, key_blk, scale), masked_score)
                new_max = jnp.maximum(run_max, jnp.max(scores, axis=1))
                weights = jnp.where(allowed, jnp.exp(scores - new_max[:, None]), 0.0)
                return (new_max, run_sum * jnp.exp(run_max - new_max) + jnp.sum(weights, axis=1))

            return lax.cond(
                block_empty(doc_row, q_start, k_start, block),
                lambda state_in: state_in,
                stats_live,
                state,
            )

        first_state = (
            jnp.full((block,), masked_score, jnp.float32),
            jnp.zeros((block,), jnp.float32),
        )
        run_max, run_sum = lax.fori_loop(0, q_block + 1, stats_step, first_state)
        lse_blk = run_max + jnp.log(run_sum)

        def value_step(k_block, acc):
            k_start = k_block * block

            def value_live(acc_in):
                key_blk = lax.dynamic_slice_in_dim(key_rows, k_start, block, 1)
                value_blk = lax.dynamic_slice_in_dim(values, k_start, block, 1)
                allowed = block_mask(doc_row, q_start, k_start, block)
                scores = block_scores(query_blk, key_blk, scale)
                probs = jnp.where(allowed, jnp.exp(scores - lse_blk[:, None]), 0.0).astype(
                    jnp.bfloat16
                )
                return acc_in + jnp.einsum(
                    "qk,ek->eq", probs, value_blk, preferred_element_type=jnp.float32
                )

            return lax.cond(
                block_empty(doc_row, q_start, k_start, block),
                lambda acc_in: acc_in,
                value_live,
                acc,
            )

        acc = lax.fori_loop(0, q_block + 1, value_step, jnp.zeros((head_dim, block), jnp.float32))
        out_acc = lax.dynamic_update_slice_in_dim(out_acc, acc.astype(jnp.bfloat16), q_start, 1)
        lse_acc = lax.dynamic_update_slice_in_dim(lse_acc, lse_blk, q_start, 0)
        return (out_acc, lse_acc)

    first_carry = (jnp.zeros((head_dim, length), jnp.bfloat16), jnp.zeros((length,), jnp.float32))
    return lax.fori_loop(0, length // block, query_step, first_carry)


def attend_back(query, key_rows, values, grad_out, lse, doc_row, block, scale):
    head_dim, length = query.shape

    def query_step(q_block, carry):
        grad_query, grad_key, grad_value = carry
        q_start = q_block * block
        query_blk = lax.dynamic_slice_in_dim(query, q_start, block, 1)
        gout_blk = lax.dynamic_slice_in_dim(grad_out, q_start, block, 1)
        lse_blk = lax.dynamic_slice_in_dim(lse, q_start, block, 0)

        def pieces(k_start):
            key_blk = lax.dynamic_slice_in_dim(key_rows, k_start, block, 1)
            value_blk = lax.dynamic_slice_in_dim(values, k_start, block, 1)
            allowed = block_mask(doc_row, q_start, k_start, block)
            scores = block_scores(query_blk, key_blk, scale)
            probs = jnp.where(allowed, jnp.exp(scores - lse_blk[:, None]), 0.0)
            dprobs = jnp.einsum(
                "eq,ek->qk", gout_blk, value_blk, preferred_element_type=jnp.float32
            )
            return (key_blk, probs, dprobs)

        def delta_step(k_block, delta):
            k_start = k_block * block

            def delta_live(delta_in):
                _, probs, dprobs = pieces(k_start)
                return delta_in + jnp.sum(probs * dprobs, axis=1)

            return lax.cond(
                block_empty(doc_row, q_start, k_start, block),
                lambda delta_in: delta_in,
                delta_live,
                delta,
            )

        delta = lax.fori_loop(0, q_block + 1, delta_step, jnp.zeros((block,), jnp.float32))

        def grad_step(k_block, state):
            k_start = k_block * block

            def grad_live(state_in):
                query_part, key_all, value_all = state_in
                key_blk, probs, dprobs = pieces(k_start)
                dscores = (probs * (dprobs - delta[:, None])).astype(jnp.bfloat16)
                query_part = query_part + jnp.einsum(
                    "qk,ek->eq", dscores, key_blk, preferred_element_type=jnp.float32
                )
                key_add = (
                    jnp.einsum("qk,eq->ek", dscores, query_blk, preferred_element_type=jnp.float32)
                    * scale
                )
                value_add = jnp.einsum(
                    "qk,eq->ek",
                    probs.astype(jnp.bfloat16),
                    gout_blk,
                    preferred_element_type=jnp.float32,
                )
                key_all = lax.dynamic_update_slice_in_dim(
                    key_all,
                    lax.dynamic_slice_in_dim(key_all, k_start, block, 1) + key_add,
                    k_start,
                    1,
                )
                value_all = lax.dynamic_update_slice_in_dim(
                    value_all,
                    lax.dynamic_slice_in_dim(value_all, k_start, block, 1) + value_add,
                    k_start,
                    1,
                )
                return (query_part, key_all, value_all)

            return lax.cond(
                block_empty(doc_row, q_start, k_start, block),
                lambda state_in: state_in,
                grad_live,
                state,
            )

        first_state = (jnp.zeros((head_dim, block), jnp.float32), grad_key, grad_value)
        query_part, grad_key, grad_value = lax.fori_loop(0, q_block + 1, grad_step, first_state)
        grad_query = lax.dynamic_update_slice_in_dim(grad_query, query_part * scale, q_start, 1)
        return (grad_query, grad_key, grad_value)

    zero_grid = jnp.zeros((head_dim, length), jnp.float32)
    grad_query, grad_key, grad_value = lax.fori_loop(
        0, length // block, query_step, (zero_grid, zero_grid, zero_grid)
    )
    return (
        grad_query.astype(jnp.bfloat16),
        grad_key.astype(jnp.bfloat16),
        grad_value.astype(jnp.bfloat16),
    )


def adam_update(weight, moment, second, grad):
    count = float(STEP)
    new_moment = first_beta * moment + (1.0 - first_beta) * grad
    new_second = second_beta * second + (1.0 - second_beta) * grad * grad
    moment_hat = new_moment / (1.0 - first_beta**count)
    second_hat = new_second / (1.0 - second_beta**count)
    new_weight = weight - learn_rate * (
        moment_hat / (jnp.sqrt(second_hat) + adam_epsilon) + weight_decay * weight
    )
    return (new_weight, new_moment, new_second)


def body(
    inputs,
    cotangent,
    doc_lengths,
    attn_weights,
    mlp_weights,
    vectors,
    hidden_bias,
    attn_moment,
    mlp_moment,
    vector_moment,
    hidden_moment,
    attn_second,
    mlp_second,
    vector_second,
    hidden_second,
):
    sequences, local_len, width_part = inputs.shape
    n_context = lax.axis_size(CONTEXT)
    n_tensor = lax.axis_size(TENSOR)
    heads_here = HEADS // n_tensor
    tokens_here = sequences * local_len
    length = local_len * n_context
    block = min(512, length)
    per_device = sequences * heads_here // n_context
    scale = HD ** (-0.5)
    half_rot = ROT // 2
    ends = jnp.cumsum(doc_lengths, axis=1)
    starts = ends - doc_lengths
    all_index = jnp.arange(length, dtype=jnp.int32)
    doc_ids = jnp.sum((all_index[None, :, None] >= ends[:, None, :]).astype(jnp.int32), axis=2)
    local_index = lax.axis_index(CONTEXT) * local_len + jnp.arange(local_len, dtype=jnp.int32)
    inside = (local_index[None, :, None] >= starts[:, None, :]) & (
        local_index[None, :, None] < ends[:, None, :]
    )
    doc_start = jnp.sum(jnp.where(inside, starts[:, None, :], 0), axis=2)
    position = (local_index[None, :] - doc_start).astype(jnp.float32)
    freq = rotary_base ** (-(2.0 * jnp.arange(half_rot, dtype=jnp.float32)) / ROT)
    angle = freq[None, :, None] * position[:, None, :]
    cosine = jnp.cos(angle)[:, None]
    sine = jnp.sin(angle)[:, None]
    norm_low = vectors[0:2].astype(jnp.bfloat16)
    tokens_full, norm_full = (
        lax.all_gather(inputs, TENSOR, axis=2, tiled=True),
        lax.all_gather(norm_low, TENSOR, axis=1, tiled=True),
    )
    rows_in = tokens_full.astype(jnp.float32).reshape(tokens_here, D)
    mean_val = jnp.mean(rows_in, axis=1, keepdims=True)
    centered = rows_in - mean_val
    variance = jnp.mean(centered * centered, axis=1, keepdims=True)
    inv_std = lax.rsqrt(variance + norm_epsilon)
    normal = centered * inv_std
    gain_full = norm_full[0].astype(jnp.float32)
    normed = (normal * gain_full + norm_full[1].astype(jnp.float32)).astype(jnp.bfloat16)
    attn_full, mlp_full = (
        lax.all_gather(attn_weights.astype(jnp.bfloat16), (SHARD, CONTEXT), axis=1, tiled=True),
        lax.all_gather(mlp_weights.astype(jnp.bfloat16), (SHARD, CONTEXT), axis=1, tiled=True),
    )
    token_grid = normed.reshape(sequences, local_len, D)
    qkv_weights = attn_full[0:3].reshape(3, D, heads_here, HD)
    projected = jnp.einsum(
        "std,cdhe->cshet", token_grid, qkv_weights, preferred_element_type=jnp.float32
    )
    query_pre = projected[0] + vectors[2].reshape(heads_here, HD)[None, :, :, None]
    key_pre = projected[1] + vectors[3].reshape(heads_here, HD)[None, :, :, None]
    value_pre = projected[2] + vectors[4].reshape(heads_here, HD)[None, :, :, None]
    outgoing = jnp.stack(
        [
            rotate(query_pre, cosine, sine, half_rot),
            rotate(key_pre, cosine, sine, half_rot),
            value_pre,
        ]
    ).astype(jnp.bfloat16)
    outgoing = outgoing.reshape(3, sequences * heads_here, HD, local_len)
    attn_in = lax.all_to_all(outgoing, CONTEXT, split_axis=1, concat_axis=3, tiled=True)
    item_index = lax.axis_index(CONTEXT) * per_device + jnp.arange(per_device, dtype=jnp.int32)
    item_docs = jnp.take(doc_ids, item_index // heads_here, axis=0)

    def attend_one(parts):
        query, key_part, value_part, doc_row = parts
        return attend_item(query, key_part, value_part, doc_row, block, scale)

    attn_out, lse = lax.map(attend_one, (attn_in[0], attn_in[1], attn_in[2], item_docs))
    heads_out = lax.all_to_all(attn_out, CONTEXT, split_axis=2, concat_axis=0, tiled=True)
    heads_grid = heads_out.reshape(sequences, heads_here, HD, local_len)
    out_weights = attn_full[3].reshape(D, heads_here, HD)
    branch = jnp.einsum(
        "shet,ohe->sto", heads_grid, out_weights, preferred_element_type=jnp.float32
    ).reshape(tokens_here, D)
    pre_act = jnp.dot(normed, mlp_full[0], preferred_element_type=jnp.float32) + hidden_bias
    gelu_value, gelu_back = jax.vjp(lambda field: jax.nn.gelu(field, approximate=True), pre_act)
    hidden = gelu_value.astype(jnp.bfloat16)
    branch = branch + jnp.einsum(
        "tf,of->to", hidden, mlp_full[1], preferred_element_type=jnp.float32
    )
    summed = lax.psum_scatter(branch, TENSOR, scatter_dimension=1, tiled=True)
    input_rows = inputs.astype(jnp.float32).reshape(tokens_here, width_part)
    output = (
        (input_rows + summed + vectors[5] + vectors[6])
        .astype(jnp.bfloat16)
        .reshape(sequences, local_len, width_part)
    )
    grad_full = lax.all_gather(cotangent, TENSOR, axis=2, tiled=True)
    grad_rows = grad_full.reshape(tokens_here, D)
    attn_back, mlp_back = (
        lax.all_gather(attn_weights.astype(jnp.bfloat16), (SHARD, CONTEXT), axis=1, tiled=True),
        lax.all_gather(mlp_weights.astype(jnp.bfloat16), (SHARD, CONTEXT), axis=1, tiled=True),
    )
    out_back = attn_back[3].reshape(D, heads_here, HD)
    grad_heads = jnp.einsum(
        "sto,ohe->shet", grad_full, out_back, preferred_element_type=jnp.float32
    ).astype(jnp.bfloat16)
    grad_heads = grad_heads.reshape(sequences * heads_here, HD, local_len)
    grad_items = lax.all_to_all(grad_heads, CONTEXT, split_axis=0, concat_axis=2, tiled=True)

    def attend_grad(parts):
        query, key_part, value_part, gout, lse_row, doc_row = parts
        return attend_back(query, key_part, value_part, gout, lse_row, doc_row, block, scale)

    grad_query_item, grad_key_item, grad_value_item = lax.map(
        attend_grad, (attn_in[0], attn_in[1], attn_in[2], grad_items, lse, item_docs)
    )
    grads_back = lax.all_to_all(
        jnp.stack([grad_query_item, grad_key_item, grad_value_item]),
        CONTEXT,
        split_axis=3,
        concat_axis=1,
        tiled=True,
    )
    grad_grid = grads_back.reshape(3, sequences, heads_here, HD, local_len)
    grad_query = rotate(grad_grid[0].astype(jnp.float32), cosine, -sine, half_rot).astype(
        jnp.bfloat16
    )
    grad_key = rotate(grad_grid[1].astype(jnp.float32), cosine, -sine, half_rot).astype(
        jnp.bfloat16
    )
    grad_proj = jnp.stack([grad_query, grad_key, grad_grid[2]])
    qkv_back = attn_back[0:3].reshape(3, D, heads_here, HD)
    qkv_grad = jnp.einsum(
        "std,cshet->cdhe", token_grid, grad_proj, preferred_element_type=jnp.float32
    ).reshape(3, D, width_part)
    normed_grad = jnp.einsum(
        "cshet,cdhe->std", grad_proj, qkv_back, preferred_element_type=jnp.float32
    ).reshape(tokens_here, D)
    out_grad = jnp.einsum(
        "sto,shet->ohe", grad_full, heads_grid, preferred_element_type=jnp.float32
    ).reshape(D, width_part)
    hidden_act_grad = jnp.dot(grad_rows, mlp_back[1], preferred_element_type=jnp.float32)
    pre_grad = gelu_back(hidden_act_grad)[0].astype(jnp.bfloat16)
    second_grad = jnp.einsum("to,tf->of", grad_rows, hidden, preferred_element_type=jnp.float32)
    first_grad = jnp.einsum("td,tf->df", normed, pre_grad, preferred_element_type=jnp.float32)
    normed_grad = normed_grad + jnp.einsum(
        "tf,df->td", pre_grad, mlp_back[0], preferred_element_type=jnp.float32
    )
    norm_stats = jnp.stack([jnp.sum(normed_grad * normal, axis=0), jnp.sum(normed_grad, axis=0)])
    scaled = normed_grad * gain_full
    input_part = inv_std * (
        scaled
        - jnp.mean(scaled, axis=1, keepdims=True)
        - normal * jnp.mean(scaled * normal, axis=1, keepdims=True)
    )
    input_slice, norm_slice = (
        lax.psum_scatter(input_part, TENSOR, scatter_dimension=1, tiled=True),
        lax.psum_scatter(norm_stats, TENSOR, scatter_dimension=1, tiled=True),
    )
    cot_rows = cotangent.astype(jnp.float32).reshape(tokens_here, width_part)
    input_grad = (
        (cot_rows + input_slice).astype(jnp.bfloat16).reshape(sequences, local_len, width_part)
    )
    cot_total = jnp.sum(cot_rows, axis=0)
    query_bias_grad = jnp.sum(grad_query.astype(jnp.float32), axis=(0, 3)).reshape(width_part)
    key_bias_grad = jnp.sum(grad_key.astype(jnp.float32), axis=(0, 3)).reshape(width_part)
    value_bias_grad = jnp.sum(grad_grid[2].astype(jnp.float32), axis=(0, 3)).reshape(width_part)
    local_vectors = jnp.stack(
        [
            norm_slice[0],
            norm_slice[1],
            query_bias_grad,
            key_bias_grad,
            value_bias_grad,
            cot_total,
            cot_total,
        ]
    )
    local_hidden = jnp.sum(pre_grad.astype(jnp.float32), axis=0)
    vector_grad, hidden_grad = lax.psum((local_vectors, local_hidden), (SHARD, CONTEXT))
    attn_local = jnp.concatenate([qkv_grad, out_grad[None]], axis=0)
    mlp_local = jnp.stack([first_grad, second_grad])
    attn_grad, mlp_grad = (
        lax.psum_scatter(attn_local, (SHARD, CONTEXT), scatter_dimension=1, tiled=True),
        lax.psum_scatter(mlp_local, (SHARD, CONTEXT), scatter_dimension=1, tiled=True),
    )
    attn_new, attn_moment_new, attn_second_new = adam_update(
        attn_weights, attn_moment, attn_second, attn_grad
    )
    mlp_new, mlp_moment_new, mlp_second_new = adam_update(
        mlp_weights, mlp_moment, mlp_second, mlp_grad
    )
    vector_new, vector_moment_new, vector_second_new = adam_update(
        vectors, vector_moment, vector_second, vector_grad
    )
    hidden_new, hidden_moment_new, hidden_second_new = adam_update(
        hidden_bias, hidden_moment, hidden_second, hidden_grad
    )
    return (
        output,
        input_grad,
        attn_grad,
        mlp_grad,
        vector_grad,
        hidden_grad,
        attn_new,
        mlp_new,
        vector_new,
        hidden_new,
        attn_moment_new,
        mlp_moment_new,
        vector_moment_new,
        hidden_moment_new,
        attn_second_new,
        mlp_second_new,
        vector_second_new,
        hidden_second_new,
    )


def attention_kernel(
    first_ref,
    q_ref,
    k_ref,
    v_ref,
    gout_ref,
    cos_ref,
    low_ref,
    high_ref,
    start_ref,
    out_ref,
    gq_ref,
    gk_ref,
    gv_ref,
    key_cat,
    value_cat,
    raw,
    dprob,
    gk_acc,
    gv_acc,
    *,
    block,
    steps,
    scale,
    half_rot,
):
    row, step = pl.program_id(0), pl.program_id(2)
    pair = q_ref.shape[1]
    lane_low = lax.broadcasted_iota(jnp.int32, (block, pair), 1) < pair // 2
    contract_last = (((1,), (1,)), ((), ()))
    contract_first = (((0,), (0,)), ((), ()))
    plain = (((1,), (0,)), ((), ()))

    def dot(a, b, dims):
        return lax.dot_general(a, b, dims, preferred_element_type=jnp.float32)

    def turn(field, start, sign):
        rows = pl.ds(start, block)
        return (
            field * cos_ref[rows, :]
            + sign * (pltpu.roll(field, pair - half_rot, 1) * low_ref[rows, :])
            + sign * (pltpu.roll(field, half_rot, 1) * high_ref[rows, :])
        )

    @pl.when(step == 0)
    def _():
        gk_acc[...] = jnp.zeros_like(gk_acc)
        gv_acc[...] = jnp.zeros_like(gv_acc)

        @pl.loop(0, steps)
        def _(j):
            at = pl.multiple_of(j * block, block)
            keys = turn(k_ref[pl.ds(at, block), :], at, 1.0)
            values = v_ref[pl.ds(at, block), :]
            for half in range(2):
                keep = lane_low if half == 0 else jnp.logical_not(lane_low)
                rows = pl.ds(pl.multiple_of(2 * at, 2 * block) + half * block, block)
                key_cat[rows, :] = jnp.where(keep, keys, 0.0).astype(jnp.bfloat16)
                value_cat[rows, :] = jnp.where(keep, values, 0.0).astype(jnp.bfloat16)

    q_at = pl.multiple_of(step * block, block)
    queries = turn(q_ref[...], q_at, 1.0).astype(jnp.bfloat16)
    queries = (queries.astype(jnp.float32) * scale).astype(jnp.bfloat16)
    gout = gout_ref[...]
    first = first_ref[row * steps + step]
    begin = start_ref[...]
    q_pos = q_at + lax.broadcasted_iota(jnp.int32, (block, block), 0)
    k_lane = lax.broadcasted_iota(jnp.int32, (block, block), 1)

    def rows_of(j):
        return pl.ds(pl.multiple_of(j * (2 * block), 2 * block), 2 * block)

    def score_step(j, tops):
        scores = dot(queries, key_cat[rows_of(j), :], contract_last)
        k_pos = j * block + k_lane
        allowed = (k_pos <= q_pos) & (k_pos >= begin)
        new_tops = []
        for half in range(2):
            part = jnp.where(allowed, scores[:, half * block : (half + 1) * block], -3e38)
            raw[j, :, half * block : (half + 1) * block] = part
            new_tops.append(jnp.maximum(tops[half], jnp.max(part, axis=1, keepdims=True)))
        return tuple(new_tops)

    low_start = jnp.full((block, 1), -3e38, jnp.float32)
    tops = lax.fori_loop(first, step + 1, score_step, (low_start, low_start))

    def weight_step(j, sums):
        dp = dot(gout, value_cat[rows_of(j), :], contract_last)
        dprob[j] = dp
        new_sums = []
        for half in range(2):
            cols = slice(half * block, (half + 1) * block)
            weights = jnp.exp(raw[j, :, cols] - tops[half])
            raw[j, :, cols] = weights
            new_sums.append(sums[2 * half] + jnp.sum(weights, axis=1, keepdims=True))
            new_sums.append(
                sums[2 * half + 1] + jnp.sum(weights * dp[:, cols], axis=1, keepdims=True)
            )
        return tuple(new_sums)

    zero = jnp.zeros((block, 1), jnp.float32)
    sums = lax.fori_loop(first, step + 1, weight_step, (zero,) * 4)
    inverse = [1.0 / sums[0], 1.0 / sums[2]]
    delta = [sums[1] * inverse[0], sums[3] * inverse[1]]

    def grad_step(j, carry):
        out_acc, gq_acc = carry
        probs, dscores = [], []
        for half in range(2):
            cols = slice(half * block, (half + 1) * block)
            full = raw[j, :, cols] * inverse[half]
            probs.append(full.astype(jnp.bfloat16))
            dscores.append((full * (dprob[j, :, cols] - delta[half])).astype(jnp.bfloat16))
        probs = jnp.concatenate(probs, axis=1)
        dscores = jnp.concatenate(dscores, axis=1)
        rows = rows_of(j)
        out_acc = out_acc + dot(probs, value_cat[rows, :], plain)
        gq_acc = gq_acc + dot(dscores, key_cat[rows, :], plain)
        gk_acc[rows, :] += dot(dscores, queries, contract_first)
        gv_acc[rows, :] += dot(probs, gout, contract_first)
        return (out_acc, gq_acc)

    blank = jnp.zeros((block, pair), jnp.float32)
    out_acc, gq_acc = lax.fori_loop(first, step + 1, grad_step, (blank, blank))
    out_ref[...] = out_acc.astype(jnp.bfloat16)
    gq_low = (gq_acc * scale).astype(jnp.bfloat16).astype(jnp.float32)
    gq_ref[...] = turn(gq_low, q_at, -1.0).astype(jnp.bfloat16)

    @pl.when(step == steps - 1)
    def _():
        @pl.loop(0, steps)
        def _(j):
            at = pl.multiple_of(j * block, block)
            top = pl.ds(pl.multiple_of(2 * at, 2 * block), block)
            bottom = pl.ds(pl.multiple_of(2 * at, 2 * block) + block, block)
            gk = jnp.where(lane_low, gk_acc[top, :], gk_acc[bottom, :])
            gk_low = gk.astype(jnp.bfloat16).astype(jnp.float32)
            gk_ref[pl.ds(at, block), :] = turn(gk_low, at, -1.0).astype(jnp.bfloat16)
            gv_ref[pl.ds(at, block), :] = jnp.where(
                lane_low, gv_acc[top, :], gv_acc[bottom, :]
            ).astype(jnp.bfloat16)


def attention(qkv_pre, gout, tables, begin, first, rows, length, block):
    width = gout.shape[1]
    pair = 2 * HD
    pairs = width // pair
    steps = length // block
    cosine, low, high = tables
    whole = pl.BlockSpec((length, pair), lambda r, h, i, f: (r, h))
    keys = pl.BlockSpec((length, pair), lambda r, h, i, f: (r, pairs + h))
    values = pl.BlockSpec((length, pair), lambda r, h, i, f: (r, 2 * pairs + h))
    part = pl.BlockSpec((block, pair), lambda r, h, i, f: (r * steps + i, h))
    table = pl.BlockSpec((length, pair), lambda r, h, i, f: (r, 0))
    shape = jax.ShapeDtypeStruct((rows * length, width), jnp.bfloat16)
    return pl.pallas_call(
        functools.partial(
            attention_kernel, block=block, steps=steps, scale=HD ** (-0.5), half_rot=ROT // 2
        ),
        out_shape=(shape,) * 4,
        grid_spec=pltpu.PrefetchScalarGridSpec(
            num_scalar_prefetch=1,
            grid=(rows, pairs, steps),
            in_specs=[
                part,
                keys,
                values,
                part,
                table,
                table,
                table,
                pl.BlockSpec((block, 1), lambda r, h, i, f: (r * steps + i, 0)),
            ],
            out_specs=[part, part, whole, whole],
            scratch_shapes=[
                pltpu.VMEM((2 * length, pair), jnp.bfloat16),
                pltpu.VMEM((2 * length, pair), jnp.bfloat16),
                pltpu.VMEM((steps, block, 2 * block), jnp.float32),
                pltpu.VMEM((steps, block, 2 * block), jnp.float32),
                pltpu.VMEM((2 * length, pair), jnp.float32),
                pltpu.VMEM((2 * length, pair), jnp.float32),
            ],
        ),
        compiler_params=pltpu.CompilerParams(
            dimension_semantics=("arbitrary", "arbitrary", "arbitrary")
        ),
        cost_estimate=pl.CostEstimate(
            flops=rows * width * length * length * 8,
            bytes_accessed=rows * length * width * 30,
            transcendentals=rows * pairs * length * length,
        ),
    )(first, qkv_pre, qkv_pre, qkv_pre, gout, cosine, low, high, begin)


MESH = pl.DeviceIdType.MESH


def flipped(index, bits):
    bit = 1
    while bit <= bits:
        if bits & bit:
            index = index + bit - 2 * bit * ((index // bit) % 2)
        bit *= 2
    return index


def gather_kernel(
    x_ref,
    g_ref,
    norm_ref,
    x_out,
    g_out,
    normed_out,
    normed_halves,
    g_halves,
    mean_out,
    inv_out,
    gain_out,
    x_buf,
    g_buf,
    normed_buf,
    normed_parts,
    g_parts,
    norm_all,
    own_sem,
    send_a,
    recv_a,
    send_n,
    recv_n,
    send_r,
    recv_r,
    send_l,
    recv_l,
    out_sem,
    *,
    n_context,
    n_tensor,
    n_block,
    rows,
    strip,
):
    c, z = lax.axis_index(CONTEXT), lax.axis_index(TENSOR)
    core = c % 2
    local_len, width = x_ref.shape[1:]
    length = local_len * n_context
    sources, buffers = (x_ref, g_ref), (x_buf, g_buf)

    def peer(k):
        return flipped(c, k)

    barrier = pltpu.get_barrier_semaphore()
    for k in range(1, n_context):
        pl.semaphore_signal(barrier, inc=1, device_id={CONTEXT: peer(k)}, device_id_type=MESH)
    for k in range(1, n_tensor):
        pl.semaphore_signal(
            barrier, inc=1, device_id={TENSOR: (z + k) % n_tensor}, device_id_type=MESH
        )
    pl.semaphore_wait(barrier, n_context + n_tensor - 2)

    def at(r, chunk):
        return pl.ds(pl.multiple_of(r * length + chunk * local_len, local_len), local_len)

    def piece(f, r, chunk, origin):
        return buffers[f].at[at(r, chunk), pl.ds(pl.multiple_of(origin * width, width), width)]

    def own_copy(f, r):
        return pltpu.make_async_copy(
            sources[f].at[c * rows + r], piece(f, r, c, z), own_sem.at[f, r]
        )

    own_norm = pltpu.make_async_copy(norm_ref, norm_all.at[z], own_sem.at[2, 0])

    def swap(f, r, k):
        return pltpu.make_async_remote_copy(
            src_ref=sources[f].at[peer(k) * rows + r],
            dst_ref=piece(f, r, c, z),
            send_sem=send_a.at[f, k - 1, r],
            recv_sem=recv_a.at[f, k - 1, r],
            device_id={CONTEXT: peer(k)},
            device_id_type=MESH,
        )

    def norm_copy(k):
        return pltpu.make_async_remote_copy(
            src_ref=norm_ref,
            dst_ref=norm_all.at[z],
            send_sem=send_n.at[k - 1],
            recv_sem=recv_n.at[k - 1],
            device_id={TENSOR: (z + k) % n_tensor},
            device_id_type=MESH,
        )

    def hop(f, r, k, d, side, step):
        origin = z - d if side > 0 else z + d
        sends, recvs = (send_r, recv_r) if side > 0 else (send_l, recv_l)
        block = piece(f, r, peer(k), origin)
        return pltpu.make_async_remote_copy(
            src_ref=block,
            dst_ref=block,
            send_sem=sends.at[f, d - step, k, r],
            recv_sem=recvs.at[f, d - step, k, r],
            device_id={TENSOR: z + side * (1 - step)},
            device_id_type=MESH,
        )

    def has(d, side):
        return z >= d if side > 0 else z + d <= n_tensor - 1

    def more(side):
        return z < n_tensor - 1 if side > 0 else z > 0

    for f in range(2):
        for r in range(rows):
            own_copy(f, r).start()
        if f == 0:
            own_norm.start()
        for k in range(1, n_context):
            for r in range(rows):
                swap(f, r, k).start()
        if f == 0:
            for k in range(1, n_tensor):
                norm_copy(k).start()
    own_norm.wait()
    for k in range(1, n_tensor):
        norm_copy(k).wait_recv()

    gain = jnp.concatenate([norm_all[j, 0:1, :] for j in range(n_tensor)], axis=1)
    shift = jnp.concatenate([norm_all[j, 1:2, :] for j in range(n_tensor)], axis=1)
    gain, shift = gain.astype(jnp.float32), shift.astype(jnp.float32)
    gain_out[...] = gain

    span = x_buf.shape[1] // n_block

    def store_parts(parts, lines, value):
        for b in range(n_block):
            cols = slice((b // 2) * span, (b // 2 + 1) * span)
            parts[(b + core) % 2, lines, cols] = value[:, b * span : (b + 1) * span]

    def finish_x(base):
        @pl.loop(0, local_len // strip)
        def _(step):
            lines = pl.ds(pl.multiple_of(base + step * strip, strip), strip)
            field = x_buf[lines, :].astype(jnp.float32)
            mean_val = jnp.mean(field, axis=1, keepdims=True)
            centered = field - mean_val
            variance = jnp.mean(centered * centered, axis=1, keepdims=True)
            inv_std = lax.rsqrt(variance + norm_epsilon)
            normed = ((centered * inv_std) * gain + shift).astype(jnp.bfloat16)
            normed_buf[lines, :] = normed
            store_parts(normed_parts, lines, normed)
            mean_out[lines, :] = mean_val
            inv_out[lines, :] = inv_std

    def finish_g(base):
        @pl.loop(0, local_len // strip)
        def _(step):
            lines = pl.ds(pl.multiple_of(base + step * strip, strip), strip)
            store_parts(g_parts, lines, g_buf[lines, :])

    def results(f, r, k):
        lines = at(r, peer(k))
        if f == 0:
            pairs = [
                (x_buf.at[lines], x_out.at[lines]),
                (normed_buf.at[lines], normed_out.at[lines]),
                (normed_parts.at[0, lines], normed_halves.at[0, lines]),
                (normed_parts.at[1, lines], normed_halves.at[1, lines]),
            ]
        else:
            pairs = [
                (g_buf.at[lines], g_out.at[lines]),
                (g_parts.at[0, lines], g_halves.at[0, lines]),
                (g_parts.at[1, lines], g_halves.at[1, lines]),
            ]
        return [
            pltpu.make_async_copy(src, dst, out_sem.at[f, k, r, i])
            for i, (src, dst) in enumerate(pairs)
        ]

    order = [(f, r, k) for f in range(2) for k in range(n_context) for r in range(rows)]

    def advance(f, r, k, d):
        if d == 0:
            if k == 0:
                own_copy(f, r).wait()
            else:
                swap(f, r, k).wait_recv()
        for side in (1, -1):
            if d > 0:

                @pl.when(has(d, side))
                def _():
                    hop(f, r, k, d, side, 1).wait_recv()

            if d < n_tensor - 1:

                @pl.when(has(d, side) & more(side))
                def _():
                    hop(f, r, k, d, side, 0).start()

    advance(*order[0], 0)
    for i, (f, r, k) in enumerate(order):
        if i + 1 < len(order):
            advance(*order[i + 1], 0)
        for d in range(1, n_tensor):
            advance(f, r, k, d)
        base = r * length + peer(k) * local_len
        if f == 0:
            finish_x(base)
        else:
            finish_g(base)
        for copy in results(f, r, k):
            copy.start()

    for f, r, k in order:
        for d in range(n_tensor - 1):
            for side in (1, -1):

                @pl.when(has(d, side) & more(side))
                def _():
                    hop(f, r, k, d, side, 0).wait_send()

        if k > 0:
            swap(f, r, k).wait_send()
        for copy in results(f, r, k):
            copy.wait()
    for k in range(1, n_tensor):
        norm_copy(k).wait_send()


def gather_inputs(inputs, cotangent, norm_low, n_context, n_tensor, n_block):
    sequences, local_len, width = inputs.shape
    rows = sequences // n_context
    tokens = sequences * local_len
    full = width * n_tensor
    wide, low = jnp.float32, jnp.bfloat16
    dma = pltpu.SemaphoreType.DMA
    inside = pl.BlockSpec(memory_space=pltpu.VMEM)
    outside = pl.BlockSpec(memory_space=pl.ANY)
    hops = (2, n_tensor - 1, n_context, rows)
    return pl.pallas_call(
        functools.partial(
            gather_kernel,
            n_context=n_context,
            n_tensor=n_tensor,
            n_block=n_block,
            rows=rows,
            strip=min(32, local_len),
        ),
        out_shape=(
            jax.ShapeDtypeStruct((tokens, full), low),
            jax.ShapeDtypeStruct((tokens, full), low),
            jax.ShapeDtypeStruct((tokens, full), low),
            jax.ShapeDtypeStruct((2, tokens, full // 2), low),
            jax.ShapeDtypeStruct((2, tokens, full // 2), low),
            jax.ShapeDtypeStruct((tokens, 1), wide),
            jax.ShapeDtypeStruct((tokens, 1), wide),
            jax.ShapeDtypeStruct((1, full), wide),
        ),
        in_specs=[inside] * 3,
        out_specs=(outside,) * 5 + (inside,) * 3,
        scratch_shapes=[
            pltpu.VMEM((tokens, full), low),
            pltpu.VMEM((tokens, full), low),
            pltpu.VMEM((tokens, full), low),
            pltpu.VMEM((2, tokens, full // 2), low),
            pltpu.VMEM((2, tokens, full // 2), low),
            pltpu.VMEM((n_tensor, 2, width), low),
            dma((3, rows)),
            dma((2, n_context - 1, rows)),
            dma((2, n_context - 1, rows)),
            dma((n_tensor - 1,)),
            dma((n_tensor - 1,)),
            dma(hops),
            dma(hops),
            dma(hops),
            dma(hops),
            dma((2, n_context, rows, 4)),
        ],
        compiler_params=pltpu.CompilerParams(collective_id=0, has_side_effects=True),
    )(inputs, cotangent, norm_low)


def total_kernel(
    stats_ref,
    rest_ref,
    out_ref,
    parts,
    every,
    send_z,
    recv_z,
    send_p,
    recv_p,
    *,
    n_shard,
    n_context,
    n_tensor,
):
    y, c, z = lax.axis_index(SHARD), lax.axis_index(CONTEXT), lax.axis_index(TENSOR)
    me = y * n_context + c
    group = n_shard * n_context
    kept = stats_ref.shape[1]

    barrier = pltpu.get_barrier_semaphore()
    for k in range(1, n_tensor):
        pl.semaphore_signal(
            barrier, inc=1, device_id={TENSOR: (z + k) % n_tensor}, device_id_type=MESH
        )

    def place(k):
        other = (me + k) % group
        return {SHARD: other // n_context, CONTEXT: other % n_context}

    for k in range(1, group):
        pl.semaphore_signal(barrier, inc=1, device_id=place(k), device_id_type=MESH)
    pl.semaphore_wait(barrier, n_tensor + group - 2)

    def slice_copy(k):
        return pltpu.make_async_remote_copy(
            src_ref=stats_ref.at[(z + k) % n_tensor],
            dst_ref=parts.at[k],
            send_sem=send_z.at[k],
            recv_sem=recv_z.at[k],
            device_id={TENSOR: (z + k) % n_tensor},
            device_id_type=MESH,
        )

    for k in range(1, n_tensor):
        slice_copy(k).start()
    every[me, kept:, :] = rest_ref[...]
    total = stats_ref[z]
    for k in range(1, n_tensor):
        slice_copy(k).wait_recv()
        total = total + parts[k]
    every[me, 0:kept, :] = total

    def spread(k):
        return pltpu.make_async_remote_copy(
            src_ref=every.at[me],
            dst_ref=every.at[me],
            send_sem=send_p.at[k],
            recv_sem=recv_p.at[k],
            device_id=place(k),
            device_id_type=MESH,
        )

    def spread_from(k):
        other = (me + group - k) % group
        return pltpu.make_async_remote_copy(
            src_ref=every.at[other],
            dst_ref=every.at[other],
            send_sem=send_p.at[k],
            recv_sem=recv_p.at[k],
            device_id=place(k),
            device_id_type=MESH,
        )

    for k in range(1, group):
        spread(k).start()
    for k in range(1, group):
        spread_from(k).wait_recv()
    total = every[0]
    for j in range(1, group):
        total = total + every[j]
    out_ref[...] = total
    for k in range(1, n_tensor):
        slice_copy(k).wait_send()
    for k in range(1, group):
        spread(k).wait_send()


def total_vectors(stats, rest, n_shard, n_context, n_tensor):
    kept, (more, width) = stats.shape[1], rest.shape
    group = n_shard * n_context
    dma = pltpu.SemaphoreType.DMA
    inside = pl.BlockSpec(memory_space=pltpu.VMEM)
    return pl.pallas_call(
        functools.partial(
            total_kernel, n_shard=n_shard, n_context=n_context, n_tensor=n_tensor
        ),
        out_shape=jax.ShapeDtypeStruct((kept + more, width), jnp.float32),
        in_specs=[inside] * 2,
        out_specs=inside,
        scratch_shapes=[
            pltpu.VMEM((n_tensor, kept, width), jnp.float32),
            pltpu.VMEM((group, kept + more, width), jnp.float32),
            dma((n_tensor,)),
            dma((n_tensor,)),
            dma((group,)),
            dma((group,)),
        ],
        compiler_params=pltpu.CompilerParams(collective_id=1, has_side_effects=True),
    )(stats, rest)


def return_kernel(sum_ref, base_ref, out_ref, mixed, send, recv, own, *, n_context, rows):
    c = lax.axis_index(CONTEXT)
    local_len = out_ref.shape[1]
    length = local_len * n_context

    def peer(k):
        return flipped(c, k)

    barrier = pltpu.get_barrier_semaphore()
    for k in range(1, n_context):
        pl.semaphore_signal(barrier, inc=1, device_id={CONTEXT: peer(k)}, device_id_type=MESH)

    def lines(r, k):
        return pl.ds(pl.multiple_of(r * length + peer(k) * local_len, local_len), local_len)

    def swap(r, k, place):
        return pltpu.make_async_remote_copy(
            src_ref=mixed.at[lines(r, k)],
            dst_ref=out_ref.at[place * rows + r],
            send_sem=send.at[k, r],
            recv_sem=recv.at[k, r],
            device_id={CONTEXT: peer(k)},
            device_id_type=MESH,
        )

    def blend(r, k):
        at = lines(r, k)
        mixed[at, :] = (
            sum_ref[at, :].astype(jnp.float32) + base_ref[at, :].astype(jnp.float32)
        ).astype(jnp.bfloat16)

    order = [(r, k) for k in range(n_context - 1, -1, -1) for r in range(rows)]
    for r, k in order:
        blend(r, k)
        if (r, k) == order[0]:
            pl.semaphore_wait(barrier, n_context - 1)
        if k > 0:
            swap(r, k, c).start()
        else:
            pltpu.make_async_copy(
                mixed.at[lines(r, 0)], out_ref.at[c * rows + r], own.at[r]
            ).start()
    for r, k in order:
        if k > 0:
            swap(r, k, peer(k)).wait_recv()
            swap(r, k, c).wait_send()
        else:
            pltpu.make_async_copy(
                mixed.at[lines(r, 0)], out_ref.at[c * rows + r], own.at[r]
            ).wait()


def return_rows(summed, base, n_context, rows):
    tokens, width = summed.shape
    local_len = tokens // (rows * n_context)
    dma = pltpu.SemaphoreType.DMA
    inside = pl.BlockSpec(memory_space=pltpu.VMEM)
    return pl.pallas_call(
        functools.partial(return_kernel, n_context=n_context, rows=rows),
        out_shape=jax.ShapeDtypeStruct((n_context * rows, local_len, width), jnp.bfloat16),
        in_specs=[inside] * 2,
        out_specs=inside,
        scratch_shapes=[
            pltpu.VMEM((tokens, width), jnp.bfloat16),
            dma((n_context, rows)),
            dma((n_context, rows)),
            dma((rows,)),
        ],
        compiler_params=pltpu.CompilerParams(collective_id=2, has_side_effects=True),
    )(summed, base)


def permute(field, axis, pairs):
    return lax.ppermute(field, axis, pairs)


def pick(field, index, axis):
    return lax.dynamic_index_in_dim(field, index, axis, keepdims=False)


def fast_body(
    inputs,
    cotangent,
    doc_lengths,
    attn_weights,
    mlp_weights,
    vectors,
    hidden_bias,
    attn_moment,
    mlp_moment,
    vector_moment,
    hidden_moment,
    attn_second,
    mlp_second,
    vector_second,
    hidden_second,
):
    sequences, local_len, width = inputs.shape
    n_context, n_tensor = lax.axis_size(CONTEXT), lax.axis_size(TENSOR)
    n_shard = lax.axis_size(SHARD)
    rows = sequences // n_context
    length = local_len * n_context
    tokens = rows * length
    block = min(256, length)
    half_rot = ROT // 2
    low_type = jnp.bfloat16
    wide = jnp.float32
    at_tensor, at_context = lax.axis_index(TENSOR), lax.axis_index(CONTEXT)
    at_y, at_x = lax.axis_index(SHARD), at_context // 2
    flip_core = [(i, i ^ 1) for i in range(n_context)]
    flip_x = [(i, i ^ 2) for i in range(n_context)]
    flip_y = [(i, i ^ 1) for i in range(n_shard)]

    def dot(a, b, left, right):
        return lax.dot_general(a, b, (((left,), (right,)), ((), ())), preferred_element_type=wide)

    attn_low = jnp.concatenate([attn_weights[i] for i in range(4)], axis=1).astype(low_type)
    attn_full = lax.all_gather(attn_low, (SHARD, CONTEXT), axis=0, tiled=True)
    mlp_full = lax.all_gather(
        mlp_weights.astype(low_type), (SHARD, CONTEXT), axis=1, tiled=True
    )
    w_qkv, w_out = attn_full[:, : 3 * width], attn_full[:, 3 * width :]
    w_up, w_down = mlp_full[0], mlp_full[1]

    x_full, g_full, normed, normed_halves, g_halves, mean_val, inv_std, gain_full = gather_inputs(
        inputs,
        cotangent,
        vectors[0:2].astype(low_type),
        n_context,
        n_tensor,
        n_shard * n_context,
    )

    ends = jnp.cumsum(doc_lengths, axis=1)
    my_ends = lax.dynamic_slice_in_dim(ends, at_context * rows, rows, 0)
    index = jnp.arange(length, dtype=jnp.int32)
    doc_start = jnp.max(
        jnp.where(index[None, :, None] >= my_ends[:, None, :], my_ends[:, None, :], 0), axis=2
    )
    first = (doc_start[:, ::block] // block).reshape(-1)
    begin = doc_start.reshape(tokens, 1)
    position = (index[None, :] - doc_start).astype(wide).reshape(tokens, 1)
    lane = jnp.arange(2 * HD, dtype=jnp.int32) % HD
    freq = rotary_base ** (-(2.0 * (lane % half_rot).astype(wide)) / ROT)
    angle = position * freq[None, :]
    cosine, sine = jnp.cos(angle), jnp.sin(angle)
    tables = (
        jnp.where(lane < ROT, cosine, 1.0),
        jnp.where(lane < half_rot, -sine, 0.0),
        jnp.where((lane >= half_rot) & (lane < ROT), sine, 0.0),
    )

    qkv_pre = dot(normed, w_qkv, 1, 0) + vectors[2:5].reshape(3 * width)
    gout = dot(g_full, w_out, 1, 0).astype(low_type)
    pre_act = dot(normed, w_up, 1, 0) + hidden_bias
    gelu_value, gelu_back = jax.vjp(lambda field: jax.nn.gelu(field, approximate=True), pre_act)
    hidden = gelu_value.astype(low_type)

    attended, g_query, g_key, g_value = attention(
        qkv_pre, gout, tables, begin, first, rows, length, block
    )
    g_qkv = jnp.concatenate([g_query, g_key, g_value], axis=1)

    def scatter_features(field):
        return lax.psum_scatter(field, TENSOR, scatter_dimension=1, tiled=True)

    def own_features(field, kind):
        return lax.dynamic_slice_in_dim(field, at_tensor * width, width, 1).astype(kind)

    def back_rows(field):
        pieces = field.reshape(rows, n_context, local_len, width)
        result = jnp.zeros((n_context, rows, local_len, width), field.dtype)
        for k in range(n_context):
            piece = pick(pieces, at_context ^ k, 1)
            if k > 0:
                piece = permute(piece, CONTEXT, [(i, i ^ k) for i in range(n_context)])
            result = lax.dynamic_update_index_in_dim(result, piece, at_context ^ k, 0)
        return result.reshape(sequences, local_len, width)

    branch = (dot(attended, w_out, 1, 1) + dot(hidden, w_down, 1, 1)).astype(low_type)
    summed = scatter_features(branch)

    pre_grad = gelu_back(dot(g_full, w_down, 1, 0))[0].astype(low_type)
    local_hidden = jnp.sum(pre_grad.astype(wide), axis=0)

    def both(a, b, where):
        return pick(a, where, 0).astype(wide) + pick(b, where, 0).astype(wide)

    def core_send(parts, right):
        return dot(parts[1], right, 0, 0).astype(low_type)

    def chip_send(parts, right, sent):
        half = right.shape[1] // 2
        arrived = permute(sent, CONTEXT, flip_core)
        chip = dot(parts[0], right, 0, 0) + arrived
        chip = chip.astype(low_type).reshape(n_shard, n_context // 2, -1, right.shape[1])
        first_half, second_half = chip[..., :half], chip[..., half:]
        return (
            pick(first_half, at_x, 1),
            pick(second_half, at_y, 0),
            pick(first_half, 1 - at_x, 1),
            pick(second_half, 1 - at_y, 0),
        )

    def line_send(chip):
        kept_x, kept_y, for_x, for_y = chip
        from_x = permute(for_x, CONTEXT, flip_x)
        from_y = permute(for_y, SHARD, flip_y)
        for_y = both(kept_x, from_x, 1 - at_y).astype(low_type)
        for_x = both(kept_y, from_y, 1 - at_x).astype(low_type)
        return (kept_x, from_x, kept_y, from_y), for_y, for_x

    def own_rows(line):
        (kept_x, from_x, kept_y, from_y), for_y, for_x = line
        next_y = permute(for_y, SHARD, flip_y)
        next_x = permute(for_x, CONTEXT, flip_x)
        return jnp.concatenate(
            [both(kept_x, from_x, at_y) + next_y, both(kept_y, from_y, at_x) + next_x], axis=1
        )

    down_sent = core_send(g_halves, hidden)
    up_sent = core_send(normed_halves, pre_grad)
    qkv_part = dot(g_qkv, w_qkv, 1, 1)
    down_chip = chip_send(g_halves, hidden, down_sent)
    up_chip = chip_send(normed_halves, pre_grad, up_sent)

    normed_grad = dot(pre_grad, w_up, 1, 1) + qkv_part
    normal = (x_full.astype(wide) - mean_val) * inv_std
    norm_stats = jnp.stack([jnp.sum(normed_grad * normal, axis=0), jnp.sum(normed_grad, axis=0)])
    scaled = normed_grad * gain_full
    input_part = (
        inv_std
        * (
            scaled
            - jnp.mean(scaled, axis=1, keepdims=True)
            - normal * jnp.mean(scaled * normal, axis=1, keepdims=True)
        )
    ).astype(low_type)
    input_slice = scatter_features(input_part)

    qkv_sent = core_send(normed_halves, g_qkv)
    out_sent = core_send(g_halves, attended)
    qkv_chip = chip_send(normed_halves, g_qkv, qkv_sent)
    out_chip = chip_send(g_halves, attended, out_sent)
    output = own_features(x_full, wide) + summed.astype(wide) + vectors[5] + vectors[6]
    output = output.astype(low_type)
    output = back_rows(output)
    down_line = line_send(down_chip)
    up_line = line_send(up_chip)
    qkv_line = line_send(qkv_chip)
    out_line = line_send(out_chip)
    down_grad, up_grad = own_rows(down_line), own_rows(up_line)
    qkv_grad, out_grad = own_rows(qkv_line), own_rows(out_line)

    g_own = own_features(g_full, low_type)
    input_grad = return_rows(input_slice, g_own, n_context, rows)

    stats_grid = norm_stats.reshape(2, n_tensor, width).transpose(1, 0, 2)
    rest = jnp.concatenate(
        [
            jnp.sum(g_qkv.astype(wide), axis=0).reshape(3, width),
            jnp.sum(own_features(g_full, wide), axis=0)[None],
            local_hidden.reshape(-1, width),
        ]
    )
    stats_grid, rest = lax.optimization_barrier((stats_grid, rest))
    totals = total_vectors(stats_grid, rest, n_shard, n_context, n_tensor)
    vector_grad = jnp.concatenate([totals[0:6], totals[5:6]])
    hidden_grad = totals[6:].reshape(-1)

    attn_grad = jnp.stack(
        [qkv_grad[:, i * width : (i + 1) * width] for i in range(3)] + [out_grad]
    )
    mlp_grad = jnp.stack([up_grad, down_grad])
    attn_new, attn_moment_new, attn_second_new = adam_update(
        attn_weights, attn_moment, attn_second, attn_grad
    )
    mlp_new, mlp_moment_new, mlp_second_new = adam_update(
        mlp_weights, mlp_moment, mlp_second, mlp_grad
    )
    vector_new, vector_moment_new, vector_second_new = adam_update(
        vectors, vector_moment, vector_second, vector_grad
    )
    hidden_new, hidden_moment_new, hidden_second_new = adam_update(
        hidden_bias, hidden_moment, hidden_second, hidden_grad
    )
    return (
        output,
        input_grad,
        attn_grad,
        mlp_grad,
        vector_grad,
        hidden_grad,
        attn_new,
        mlp_new,
        vector_new,
        hidden_new,
        attn_moment_new,
        mlp_moment_new,
        vector_moment_new,
        hidden_moment_new,
        attn_second_new,
        mlp_second_new,
        vector_second_new,
        hidden_second_new,
    )


def row_local(n_shard, n_context):
    return n_shard == 2 and n_context == 4


def layer(*arrays):
    n_shard, n_context = lax.axis_size(SHARD), lax.axis_size(CONTEXT)
    if row_local(n_shard, n_context) and arrays[0].shape[0] % n_context == 0:
        return fast_body(*arrays)
    return body(*arrays)


def solution(mesh):
    return jax.shard_map(
        layer,
        mesh=mesh,
        in_specs=(
            P(SHARD, CONTEXT, TENSOR),
            P(SHARD, CONTEXT, TENSOR),
            P(SHARD, None),
            P(None, (SHARD, CONTEXT), TENSOR),
            P(None, (SHARD, CONTEXT), TENSOR),
            P(None, TENSOR),
            P(TENSOR),
            P(None, (SHARD, CONTEXT), TENSOR),
            P(None, (SHARD, CONTEXT), TENSOR),
            P(None, TENSOR),
            P(TENSOR),
            P(None, (SHARD, CONTEXT), TENSOR),
            P(None, (SHARD, CONTEXT), TENSOR),
            P(None, TENSOR),
            P(TENSOR),
        ),
        out_specs=(
            P(SHARD, CONTEXT, TENSOR),
            P(SHARD, CONTEXT, TENSOR),
            P(None, (SHARD, CONTEXT), TENSOR),
            P(None, (SHARD, CONTEXT), TENSOR),
            P(None, TENSOR),
            P(TENSOR),
            P(None, (SHARD, CONTEXT), TENSOR),
            P(None, (SHARD, CONTEXT), TENSOR),
            P(None, TENSOR),
            P(TENSOR),
            P(None, (SHARD, CONTEXT), TENSOR),
            P(None, (SHARD, CONTEXT), TENSOR),
            P(None, TENSOR),
            P(TENSOR),
            P(None, (SHARD, CONTEXT), TENSOR),
            P(None, (SHARD, CONTEXT), TENSOR),
            P(None, TENSOR),
            P(TENSOR),
        ),
        check_vma=False,
    )
```
